128 devices in a mesh: fsdp: 16 (over z, y), model: 8 (over x, core).
Axes of the slice: x: 4, y: 4, z: 4, core: 2. Of those that a mesh axis runs over, the one named last changes fastest.
Arguments:
- x_in: bfloat16 [128, 64, 4096], P('fsdp', 'model')
- gain_attn: float32 [2, 4096], replicated
- gain_mlp: float32 [2, 4096], replicated
- rope_cos: float32 [64, 64], replicated
- rope_sin: float32 [64, 64], replicated
- w_q: bfloat16 [2, 4096, 4096], P(None, 'fsdp', 'model')
- w_k: bfloat16 [2, 4096, 1024], P(None, 'fsdp', 'model')
- w_v: bfloat16 [2, 4096, 1024], P(None, 'fsdp', 'model')
- w_o: bfloat16 [2, 4096, 4096], P(None, 'model', 'fsdp')
- w_gate: bfloat16 [2, 4096, 14336], P(None, 'fsdp', 'model')
- w_up: bfloat16 [2, 4096, 14336], P(None, 'fsdp', 'model')
- w_down: bfloat16 [2, 14336, 4096], P(None, 'model', 'fsdp')
Outputs:
- output: bfloat16 [128, 64, 4096], P('fsdp', 'model')
All inputs are finite; a program needn't handle non-finite values.
Results may differ from the reference program's by a relative error of at most 0.02.
Values are sent between devices in bfloat16 or wider.
A program may use at most 1 GiB of HBM per device.

```python
import math
import jax
import jax.numpy as jnp
from jax import lax

D_MODEL = 4096
FFN = 14336
HEADS = 32
KV_HEADS = 8
HEAD_DIM = 128
BATCH = 128
SEQ = 64
LAYERS = 2
EPS = 1e-5
ROPE_BASE = 500000.0


def rope_tables(rng_key):
    pos_steps = jax.random.randint(rng_key, (SEQ,), 1, 4)
    positions = (jnp.cumsum(pos_steps) - pos_steps[0]).astype(jnp.float32)
    inv_freq = ROPE_BASE ** (-jnp.arange(HEAD_DIM // 2, dtype=jnp.float32) * (2.0 / HEAD_DIM))
    angles = positions[:, None] * inv_freq[None, :]
    return jnp.cos(angles), jnp.sin(angles)


def setup_inputs(seed: int = 0) -> dict:
    key_list = jax.random.split(jax.random.key(seed), 12)
    q_scale = math.sqrt(max(1.0, math.log(SEQ / 16.0)))

    def normal(rng_key, arr_shape, std_scale):
        return (jax.random.normal(rng_key, arr_shape, jnp.float32) * std_scale).astype(jnp.bfloat16)

    rope_cos, rope_sin = rope_tables(key_list[3])
    return {
        'x_in': normal(key_list[0], (BATCH, SEQ, D_MODEL), 1.0),
        'gain_attn': jax.random.uniform(key_list[1], (LAYERS, D_MODEL), jnp.float32, 0.5, 1.5),
        'gain_mlp': jax.random.uniform(key_list[2], (LAYERS, D_MODEL), jnp.float32, 0.5, 1.5),
        'rope_cos': rope_cos,
        'rope_sin': rope_sin,
        'w_q': normal(key_list[4], (LAYERS, D_MODEL, HEADS * HEAD_DIM), q_scale * D_MODEL ** -0.5),
        'w_k': normal(key_list[5], (LAYERS, D_MODEL, KV_HEADS * HEAD_DIM), D_MODEL ** -0.5),
        'w_v': normal(key_list[6], (LAYERS, D_MODEL, KV_HEADS * HEAD_DIM), D_MODEL ** -0.5),
        'w_o': normal(key_list[7], (LAYERS, HEADS * HEAD_DIM, D_MODEL), 2.0 * (HEADS * HEAD_DIM) ** -0.5),
        'w_gate': normal(key_list[8], (LAYERS, D_MODEL, FFN), D_MODEL ** -0.5),
        'w_up': normal(key_list[9], (LAYERS, D_MODEL, FFN), D_MODEL ** -0.5),
        'w_down': normal(key_list[10], (LAYERS, FFN, D_MODEL), FFN ** -0.5),
    }


def rms_norm(seq_rows, gain_vec):
    rows_f = seq_rows.astype(jnp.float32)
    mean_sq = jnp.mean(rows_f * rows_f, axis=-1, keepdims=True)
    return (rows_f * lax.rsqrt(mean_sq + EPS) * gain_vec).astype(jnp.bfloat16)


def rotate(head_vals, cos_b, sin_b):
    half_dim = head_vals.shape[-1] // 2
    heads_f = head_vals.astype(jnp.float32)
    first_half = heads_f[..., :half_dim]
    second_half = heads_f[..., half_dim:]
    return jnp.concatenate([first_half * cos_b - second_half * sin_b, second_half * cos_b + first_half * sin_b], axis=-1).astype(jnp.bfloat16)


def decoder_layer(seq_rows, params, rope_cos, rope_sin):
    gain_attn, gain_mlp, w_q, w_k, w_v, w_o, w_gate, w_up, w_down = params
    group_size = HEADS // KV_HEADS
    normed = rms_norm(seq_rows, gain_attn)
    q_proj = jnp.dot(normed, w_q, preferred_element_type=jnp.float32).astype(jnp.bfloat16).reshape(SEQ, KV_HEADS, group_size, HEAD_DIM)
    k_proj = jnp.dot(normed, w_k, preferred_element_type=jnp.float32).astype(jnp.bfloat16).reshape(SEQ, KV_HEADS, HEAD_DIM)
    v_proj = jnp.dot(normed, w_v, preferred_element_type=jnp.float32).astype(jnp.bfloat16).reshape(SEQ, KV_HEADS, HEAD_DIM)
    q_rot = rotate(q_proj, rope_cos[:, None, None, :], rope_sin[:, None, None, :])
    k_rot = rotate(k_proj, rope_cos[:, None, :], rope_sin[:, None, :])
    scores = jnp.einsum('qkgd,skd->kgqs', q_rot.astype(jnp.float32), k_rot.astype(jnp.float32)) * HEAD_DIM ** -0.5
    positions = jnp.arange(SEQ)
    causal = positions[:, None] >= positions[None, :]
    scores = jnp.where(causal, scores, -jnp.inf)
    attn_probs = jax.nn.softmax(scores, axis=-1).astype(jnp.bfloat16)
    attn_out = jnp.einsum('kgqs,skd->qkgd', attn_probs.astype(jnp.float32), v_proj.astype(jnp.float32)).astype(jnp.bfloat16).reshape(SEQ, HEADS * HEAD_DIM)
    attn_sum = jnp.dot(attn_out, w_o, preferred_element_type=jnp.float32)
    mid_rows = (seq_rows.astype(jnp.float32) + attn_sum).astype(jnp.bfloat16)
    normed_mlp = rms_norm(mid_rows, gain_mlp)
    gate_acc = jnp.dot(normed_mlp, w_gate, preferred_element_type=jnp.float32)
    up_acc = jnp.dot(normed_mlp, w_up, preferred_element_type=jnp.float32)
    hidden = (jax.nn.silu(gate_acc) * up_acc).astype(jnp.bfloat16)
    mlp_sum = jnp.dot(hidden, w_down, preferred_element_type=jnp.float32)
    return (mid_rows.astype(jnp.float32) + mlp_sum).astype(jnp.bfloat16)


def reference(x_in, gain_attn, gain_mlp, rope_cos, rope_sin, w_q, w_k, w_v, w_o, w_gate, w_up, w_down):
    params = (gain_attn, gain_mlp, w_q, w_k, w_v, w_o, w_gate, w_up, w_down)

    def one_sequence(seq_rows):
        def layer_step(carry_rows, layer_params):
            return decoder_layer(carry_rows, layer_params, rope_cos, rope_sin), None
        final_rows, _ = lax.scan(layer_step, seq_rows, params)
        return final_rows

    return lax.map(one_sequence, x_in)
```

```python
import functools
import jax
import jax.numpy as jnp
from jax import lax
from jax.experimental import pallas as pl
from jax.experimental.pallas import tpu as pltpu
from jax.sharding import PartitionSpec as P

EPS = 1e-5
MESH = pl.DeviceIdType.MESH
FULL = slice(None)

UNITS = 26
ITEMS = 13
N_ITEMS = 2 * ITEMS
KV = 2
O_BASE = 3
GU_BASE = 5
D_BASE = 19
RING = 4
LANE = 128
UNIT = 256
ROWS = 512
TOK = 64
HEAD_SCALE = 128 ** -0.5
BOTH = (0, 1)
SIGNS = (1, -1)


def _plan():
    plan = []

    def add(stage, src, sub, half, axis, sign):
        dst = list(src)
        dst[axis] -= sign
        rel = [(v[0] % RING) * RING + v[1] % RING for v in (src, dst)]
        quarters = {(a, b) for a in BOTH for b in BOTH if sub in (a, None) and half in (b, None)}
        plan.append(dict(stage=stage, src=rel[0], dst=rel[1], sub=sub, half=half, dir=(axis, sign), q=quarters))

    for axis in BOTH:
        for sign in SIGNS:
            sub = (1 - sign) // 2

            def at(along, across):
                return (along, across) if axis == 0 else (across, along)

            add(0, at(0, 0), None, None, axis, sign)
            add(1, at(-sign, 0), sub, None, axis, sign)
            for k in SIGNS:
                add(1, at(0, k), None, axis, axis, sign)
                add(2, at(-sign, k), sub, axis, axis, sign)
            add(2, at(0, 2), None, axis, axis, sign)
            add(3, at(-sign, 2), sub, axis, axis, sign)
    return plan


PLAN = _plan()
N_COPY = len(PLAN)


def _pick(sub, half):
    return (FULL if sub is None else pl.ds(sub, 1), FULL if half is None else pl.ds(half, 1))


def body(x_ref, ga_ref, gm_ref, cos_ref, sin_ref, wq, wk, wv, wo, wg, wu, wd, y_ref, g_ref,
         hu, wbuf, dbuf, part, t1, t2, t3, zbuf, qbuf, kbuf, vbuf, obuf, res, acc_a, acc_b,
         st_recv, st_send, ag_recv, ag_send, rs_recv, rs_send, w_sem, d_sem):
    f_me = lax.axis_index("fsdp")
    m_me = lax.axis_index("model")
    z, y = lax.div(f_me, 4), lax.rem(f_me, 4)
    x, c = lax.div(m_me, 2), lax.rem(m_me, 2)
    up = lambda v: lax.rem(v + 1, 4)
    dn = lambda v: lax.rem(v + 3, 4)
    sib = 1 - c

    dev_of = {}
    for s, turn in zip(SIGNS, (up, dn)):
        dev_of[0, s] = (turn(z) * 4 + y, m_me)
        dev_of[1, s] = (z * 4 + turn(y), m_me)
    x_up, x_dn, x_far = up(x), dn(x), lax.rem(x + 2, 4)
    dev_xu, dev_xd, dev_sib = (f_me, x_up * 2 + c), (f_me, x_dn * 2 + c), (f_me, x * 2 + sib)

    def stream_copy(item, i):
        p = PLAN[i]
        a, b = _pick(p["sub"], p["half"])
        u = pl.ds(2 * item, 2)
        at = p["src"] if p["stage"] else p["dst"]
        src = g_ref.at[u, at, a, b]
        return pltpu.make_async_remote_copy(
            src_ref=src, dst_ref=g_ref.at[u, p["dst"], a, b],
            send_sem=st_send.at[item], recv_sem=st_recv.at[item, i],
            device_id=dev_of[p["dir"]], device_id_type=MESH)

    def arrivals(stage):
        return [i for i in range(N_COPY) if PLAN[i]["stage"] == stage]

    def start_unit(item, e):
        unit = 2 * item + e
        layer, ul = lax.div(unit, UNITS), lax.rem(unit, UNITS)

        def send(src, lane=None):
            for i in arrivals(0):
                dst = g_ref.at[unit, PLAN[i]["dst"]]
                pltpu.make_async_remote_copy(
                    src_ref=src, dst_ref=dst if lane is None else dst.at[:, :, :, pl.ds(lane, LANE)],
                    send_sem=st_send.at[item], recv_sem=st_recv.at[item, i],
                    device_id=dev_of[PLAN[i]["dir"]], device_id_type=MESH).start()

        @pl.when(ul < KV)
        def _():
            send(own_cols(wq, layer, ul))

        @pl.when(ul == KV)
        def _():
            send(wk.at[layer], 0)
            send(wv.at[layer], LANE)

        for w, lo, hi, n_row in ((wo, O_BASE, GU_BASE, 2), (wd, D_BASE, UNITS, 7)):
            @pl.when(jnp.logical_and(ul >= lo, ul < hi))
            def _():
                for k in BOTH:
                    send(own_part(w, layer, n_row, 2 * (ul - lo) + k), k * LANE)

        for k, w in enumerate((wg, wu)):
            @pl.when(jnp.logical_and(jnp.logical_and(ul >= GU_BASE, ul < D_BASE), lax.rem(ul - GU_BASE, 2) == k))
            def _():
                send(own_cols(w, layer, lax.div(ul - GU_BASE, 2)))

    def own_cols(w, layer, j):
        return w.at[layer, :, :, :, pl.ds(pl.multiple_of(j * UNIT, UNIT), UNIT)]

    def own_part(w, layer, n_row, s):
        lane = pl.multiple_of(lax.div(s, n_row) * LANE, LANE)
        return w.at[layer, lax.rem(s, n_row), :, :, :, pl.ds(lane, LANE)]

    def start_own(item):
        for e in BOTH:
            start_unit(item, e)

    def forward(item, stage):
        waited = set()
        for i in arrivals(stage):
            p = PLAN[i]
            for j in arrivals(stage - 1):
                if j not in waited and PLAN[j]["dst"] == p["src"] and PLAN[j]["q"] & p["q"]:
                    stream_copy(item, j).wait_recv()
                    waited.add(j)
            stream_copy(item, i).start()
        for j in arrivals(stage - 1):
            if j not in waited:
                stream_copy(item, j).wait_recv()

    def tick(t):
        @pl.when(t < N_ITEMS)
        def _():
            forward(t, 1)

        @pl.when(jnp.logical_and(t >= 1, t < N_ITEMS + 1))
        def _():
            forward(t - 1, 2)

        @pl.when(jnp.logical_and(t >= 2, t < N_ITEMS + 2))
        def _():
            forward(t - 2, 3)

        @pl.when(t + 2 < N_ITEMS)
        def _():
            start_own(t + 2)

        @pl.when(jnp.logical_and(t >= 3, t < N_ITEMS + 3))
        def _():
            for j in arrivals(3):
                stream_copy(t - 3, j).wait_recv()

    def ag_copy(inst, k):
        slot = lax.rem(inst, 2)
        own, lo, hi, far = (x * 2 + c), (x_dn * 2 + c), (x_up * 2 + c), (x_far * 2 + c)
        s0, s1 = pl.ds(0, 32), pl.ds(32, 32)
        blk, rows, dev = [
            (own, FULL, dev_sib), (own, FULL, dev_xu), (own, FULL, dev_xd),
            (lo, s0, dev_xu), (hi, s1, dev_xd),
            (lo, FULL, dev_sib), (hi, FULL, dev_sib), (far, FULL, dev_sib)][k]
        return pltpu.make_async_remote_copy(
            src_ref=hu.at[slot, blk, rows], dst_ref=hu.at[slot, blk, rows],
            send_sem=ag_send.at[inst, k], recv_sem=ag_recv.at[inst, k], device_id=dev, device_id_type=MESH)

    def ag_start(inst):
        for k in (1, 2, 0):
            ag_copy(inst, k).start()

    def ag_mid(inst):
        ag_copy(inst, 1).wait_recv()
        ag_copy(inst, 3).start()
        ag_copy(inst, 5).start()
        ag_copy(inst, 2).wait_recv()
        ag_copy(inst, 4).start()
        ag_copy(inst, 6).start()

    def ag_end(inst):
        ag_copy(inst, 3).wait_recv()
        ag_copy(inst, 4).wait_recv()
        ag_copy(inst, 7).start()
        for k in (0, 5, 6, 7):
            ag_copy(inst, k).wait_recv()
        for k in range(8):
            ag_copy(inst, k).wait_send()

    def rs_copy(inst, hh, k):
        lo, hi = pl.ds(0, 32), pl.ds(32, 32)
        src, dst, dev = [
            (part.at[hh, :, sib], t1.at[hh], dev_sib),
            (part.at[hh, x_far, c, lo], t2.at[hh, 0], dev_xu),
            (part.at[hh, x_far, c, hi], t2.at[hh, 1], dev_xd),
            (part.at[hh, x_up, c], t3.at[hh, 0], dev_xu),
            (part.at[hh, x_dn, c], t3.at[hh, 1], dev_xd)][k]
        return pltpu.make_async_remote_copy(
            src_ref=src, dst_ref=dst, send_sem=rs_send.at[inst, hh, k], recv_sem=rs_recv.at[inst, hh, k],
            device_id=dev, device_id_type=MESH)

    def rs_core(inst, hh):
        rs_copy(inst, hh, 0).start()

    def rs_far(inst, hh):
        rs_copy(inst, hh, 0).wait_recv()

        def add(xp):
            part[hh, xp, c] = part[hh, xp, c] + t1[hh, xp]

        add(x_far)
        rs_copy(inst, hh, 1).start()
        rs_copy(inst, hh, 2).start()
        for xp in (x_up, x_dn, x):
            add(xp)

    def rs_near(inst, hh):
        rs_copy(inst, hh, 1).wait_recv()
        part[hh, x_up, c, 0:32] = part[hh, x_up, c, 0:32] + t2[hh, 0]
        rs_copy(inst, hh, 3).start()
        rs_copy(inst, hh, 2).wait_recv()
        part[hh, x_dn, c, 32:TOK] = part[hh, x_dn, c, 32:TOK] + t2[hh, 1]
        rs_copy(inst, hh, 4).start()

    def rs_wait(inst, hh):
        rs_copy(inst, hh, 3).wait_recv()
        rs_copy(inst, hh, 4).wait_recv()
        for k in range(5):
            rs_copy(inst, hh, k).wait_send()

    def add_residual():
        def rows16(i, _):
            r = pl.ds(pl.multiple_of(i * 16, 16), 16)
            s = [part[hh, x, c, r] + t3[hh, 0, r] + t3[hh, 1, r] for hh in range(2)]
            cols = []
            for f in range(16):
                for hh in range(2):
                    cols.append(s[hh][:, f * LANE:(f + 1) * LANE])
            total = jnp.concatenate(cols, axis=1)
            res[r] = (res[r].astype(jnp.float32) + total).astype(jnp.bfloat16)
            return 0
        lax.fori_loop(0, 4, rows16, 0)

    def norm_into(slot, gain):
        def rows16(i, _):
            r = pl.ds(pl.multiple_of(i * 16, 16), 16)
            v = res[r].astype(jnp.float32)
            ms = jnp.mean(v * v, axis=-1, keepdims=True)
            hu[slot, m_me, r] = (v * lax.rsqrt(ms + EPS) * gain).astype(jnp.bfloat16)
            return 0
        lax.fori_loop(0, 4, rows16, 0)

    def abs_of(rel):
        return lax.rem(z + lax.div(rel, 4), 4) * 4 + lax.rem(y + lax.rem(rel, 4), 4)

    def load_unit(unit, slot, own):
        mine = wbuf.at[slot, f_me]
        if len(own) == 1:
            pltpu.make_async_copy(own[0], mine, w_sem.at[slot]).start()
        else:
            for k in BOTH:
                pltpu.make_async_copy(own[k], mine.at[:, :, :, pl.ds(k * LANE, LANE)], w_sem.at[slot]).start()

        def one(rel, _):
            pltpu.make_async_copy(g_ref.at[unit, rel], wbuf.at[slot, abs_of(rel)], w_sem.at[slot]).start()
            return 0
        lax.fori_loop(1, 16, one, 0)

    def wait_unit(slot):
        pltpu.make_async_copy(wbuf.at[slot], wbuf.at[slot], w_sem.at[slot]).wait()

    def load_cols(w, layer, base, n_row, hh):
        def row(r, _):
            s = hh * n_row + r
            unit = layer * UNITS + base + lax.div(s, 2)
            lane = pl.ds(pl.multiple_of(lax.rem(s, 2) * LANE, LANE), LANE)

            def dst(f):
                return dbuf.at[r, :, :, :, pl.ds(pl.multiple_of(f * LANE, LANE), LANE)]
            pltpu.make_async_copy(own_part(w, layer, n_row, s), dst(f_me), d_sem).start()

            def one(rel, _):
                pltpu.make_async_copy(g_ref.at[unit, rel, :, :, :, lane], dst(abs_of(rel)), d_sem).start()
                return 0
            lax.fori_loop(1, 16, one, 0)
            return 0
        lax.fori_loop(0, n_row, row, 0)
        span = dbuf.at[pl.ds(0, n_row)]
        pltpu.make_async_copy(span, span, d_sem).wait()

    def project(slot, wslots, accs):
        for acc in accs:
            acc[...] = jnp.zeros_like(acc)

        def step(kk, _):
            lhs = hu[slot, :, :, pl.ds(pl.multiple_of(kk * ROWS, ROWS), ROWS)].reshape(ROWS, ROWS)
            for ws, acc in zip(wslots, accs):
                rhs = wbuf[ws, pl.ds(2 * kk, 2)].reshape(ROWS, UNIT)
                acc[...] += jnp.dot(lhs, rhs, preferred_element_type=jnp.float32)
            return 0
        lax.fori_loop(0, 8, step, 0)

    def rope_store(src, lane, dst):
        def rows(i, _):
            r = pl.ds(pl.multiple_of(i * LANE, LANE), LANE)
            v = src[r, lane:lane + LANE].astype(jnp.bfloat16).astype(jnp.float32)
            out = v * cos_ref[r] + pltpu.roll(v, TOK, 1) * sin_ref[r]
            dst[r] = out.astype(jnp.bfloat16)
            return 0
        lax.fori_loop(0, 4, rows, 0)

    def attention(layer):
        base = layer * UNITS
        slot = 0
        for u in BOTH:
            load_unit(base + u, u, [own_cols(wq, layer, u)])
        load_unit(base + KV, KV, [wk.at[layer], wv.at[layer]])
        wait_unit(0)
        wait_unit(1)
        project(slot, (0, 1), (acc_a, acc_b))
        for h in range(4):
            rope_store(acc_a if h < 2 else acc_b, (h % 2) * LANE, qbuf.at[h])
        wait_unit(2)
        project(slot, (2,), (acc_a,))
        rope_store(acc_a, 0, kbuf)
        vbuf[...] = acc_a[:, LANE:UNIT].astype(jnp.bfloat16)

        def rows(i, _):
            r0 = pl.multiple_of(i * LANE, LANE)
            r = pl.ds(r0, LANE)
            qi = lax.broadcasted_iota(jnp.int32, (LANE, ROWS), 0) + r0
            ki = lax.broadcasted_iota(jnp.int32, (LANE, ROWS), 1)
            same = ((qi >> 3) & 7) == ((ki >> 3) & 7)
            qpos = (qi >> 6) * 8 + (qi & 7)
            kpos = (ki >> 6) * 8 + (ki & 7)
            ok = jnp.logical_and(same, qpos >= kpos)
            for h in range(4):
                s = lax.dot_general(qbuf[h, r], kbuf[...], (((1,), (1,)), ((), ())), preferred_element_type=jnp.float32)
                s = jnp.where(ok, s * (HEAD_SCALE), -jnp.inf)
                e = jnp.exp(s - jnp.max(s, axis=-1, keepdims=True))
                p = (e / jnp.sum(e, axis=-1, keepdims=True)).astype(jnp.bfloat16)
                o = jnp.dot(p, vbuf[...], preferred_element_type=jnp.float32)
                obuf[r, h * LANE:(h + 1) * LANE] = o.astype(jnp.bfloat16)
            return 0
        lax.fori_loop(0, 4, rows, 0)

    def down(act, w, layer, n_row, base, hh):
        load_cols(w, layer, base, n_row, hh)

        def tile(n, _):
            cols = pl.ds(pl.multiple_of(n * UNIT, UNIT), UNIT)
            rhs = dbuf[0:n_row, :, :, :, cols].reshape(n_row * UNIT, UNIT)
            out = jnp.dot(act[...], rhs, preferred_element_type=jnp.float32)
            part[hh, :, :, :, cols] = out.reshape(4, 2, TOK, UNIT)
            return 0
        lax.fori_loop(0, 8, tile, 0)

    def gate_up(layer, j0, j1):
        def load(j, b):
            u = layer * UNITS + GU_BASE + 2 * j
            load_unit(u, 2 * b, [own_cols(wg, layer, j)])
            load_unit(u + 1, 2 * b + 1, [own_cols(wu, layer, j)])

        load(j0, j0 % 2)

        def step(j, _):
            b = lax.rem(j, 2)

            @pl.when(j + 1 < j1)
            def _():
                load(j + 1, 1 - b)
            wait_unit(2 * b)
            wait_unit(2 * b + 1)
            project(1, (2 * b, 2 * b + 1), (acc_a, acc_b))

            def rows(i, _):
                r = pl.ds(pl.multiple_of(i * LANE, LANE), LANE)
                hid = jax.nn.silu(acc_a[r]) * acc_b[r]
                zbuf[r, pl.ds(pl.multiple_of(j * UNIT, UNIT), UNIT)] = hid.astype(jnp.bfloat16)
                return 0
            lax.fori_loop(0, 4, rows, 0)
            return 0
        lax.fori_loop(j0, j1, step, 0)

    barrier = pltpu.get_barrier_semaphore()
    peers = list(dev_of.values()) + [dev_xu, dev_xd, dev_sib]
    for dev in peers:
        pl.semaphore_signal(barrier, inc=1, device_id=dev, device_id_type=MESH)
    pl.semaphore_wait(barrier, len(peers))

    start_own(0)
    start_own(1)
    res[...] = x_ref[...]
    norm_into(0, ga_ref[0])
    ag_start(0)

    def hooks(layer, tau):
        a_inst, m_inst = 2 * layer, 2 * layer + 1

        @pl.when(tau == 5)
        def _():
            ag_mid(a_inst)

        @pl.when(tau == 6)
        def _():
            ag_end(a_inst)
            attention(layer)
            for hh in range(2):
                down(obuf, wo, layer, 2, O_BASE, hh)
                rs_core(a_inst, hh)

        @pl.when(tau == 7)
        def _():
            for hh in range(2):
                rs_far(a_inst, hh)

        @pl.when(tau == 8)
        def _():
            for hh in range(2):
                rs_near(a_inst, hh)

        @pl.when(tau == 9)
        def _():
            for hh in range(2):
                rs_wait(a_inst, hh)
            add_residual()
            norm_into(1, gm_ref[layer])
            ag_start(m_inst)

        @pl.when(tau == 10)
        def _():
            ag_mid(m_inst)

        @pl.when(tau == 11)
        def _():
            ag_end(m_inst)
            gate_up(layer, 0, 6)

        @pl.when(tau == 12)
        def _():
            gate_up(layer, 6, 7)

        @pl.when(tau == 14)
        def _():
            down(zbuf, wd, layer, 7, D_BASE, 0)
            rs_core(m_inst, 0)

        @pl.when(tau == 15)
        def _():
            rs_far(m_inst, 0)
            down(zbuf, wd, layer, 7, D_BASE, 1)
            rs_core(m_inst, 1)

        @pl.when(tau == 16)
        def _():
            rs_near(m_inst, 0)
            rs_far(m_inst, 1)

        @pl.when(tau == 17)
        def _():
            rs_near(m_inst, 1)
            for hh in range(2):
                rs_wait(m_inst, hh)
            add_residual()

            @pl.when(layer == 0)
            def _():
                norm_into(0, ga_ref[1])
                ag_start(2)

    def step(t, _):
        tick(t)

        @pl.when(t >= 5)
        def _():
            hooks(lax.div(t - 5, ITEMS), lax.rem(t - 5, ITEMS) + 5)
        return 0
    lax.fori_loop(0, 5 + 2 * ITEMS, step, 0)
    y_ref[...] = res[...]

    def drain(i, _):
        span = g_ref.at[pl.ds(2 * i, 2), pl.ds(0, 15)]
        pltpu.make_async_copy(span, span, st_send.at[i]).wait()
        return 0
    lax.fori_loop(0, N_ITEMS, drain, 0)


def _call(x, ga, gm, cos, sin, *weights):
    bf, f32 = jnp.bfloat16, jnp.float32
    vm = pl.BlockSpec(memory_space=pltpu.VMEM)
    anys = pl.BlockSpec(memory_space=pl.ANY)
    return pl.pallas_call(
        body,
        out_shape=(jax.ShapeDtypeStruct((TOK, 4096), bf), jax.ShapeDtypeStruct((2 * UNITS, 16, 2, 2, TOK, UNIT), bf)),
        in_specs=[vm] * 5 + [anys] * len(weights),
        out_specs=(vm, anys),
        scratch_shapes=[
            pltpu.VMEM((2, 8, TOK, 4096), bf),
            pltpu.VMEM((4, 16, 2, 2, TOK, UNIT), bf),
            pltpu.VMEM((7, 2, 2, TOK, 2048), bf),
            pltpu.VMEM((2, 4, 2, TOK, 2048), f32),
            pltpu.VMEM((2, 4, TOK, 2048), f32),
            pltpu.VMEM((2, 2, 32, 2048), f32),
            pltpu.VMEM((2, 2, TOK, 2048), f32),
            pltpu.VMEM((ROWS, 1792), bf),
            pltpu.VMEM((4, ROWS, LANE), bf),
            pltpu.VMEM((ROWS, LANE), bf),
            pltpu.VMEM((ROWS, LANE), bf),
            pltpu.VMEM((ROWS, ROWS), bf),
            pltpu.VMEM((TOK, 4096), bf),
            pltpu.VMEM((ROWS, UNIT), f32),
            pltpu.VMEM((ROWS, UNIT), f32),
            pltpu.SemaphoreType.DMA((N_ITEMS, N_COPY)),
            pltpu.SemaphoreType.DMA((N_ITEMS,)),
            pltpu.SemaphoreType.DMA((4, 8)),
            pltpu.SemaphoreType.DMA((4, 8)),
            pltpu.SemaphoreType.DMA((4, 2, 5)),
            pltpu.SemaphoreType.DMA((4, 2, 5)),
            pltpu.SemaphoreType.DMA((4,)),
            pltpu.SemaphoreType.DMA,
        ],
        compiler_params=pltpu.CompilerParams(collective_id=0, has_side_effects=True, vmem_limit_bytes=62 * 1024 * 1024),
        cost_estimate=pl.CostEstimate(flops=56 * 10 ** 9, bytes_accessed=330 * 10 ** 6, transcendentals=10 ** 7),
    )(x, ga, gm, cos, sin, *weights)[0]


def solution(mesh):
    act = P('fsdp', 'model', None)
    col = P(None, 'fsdp', 'model')
    row = P(None, 'model', 'fsdp')

    def device_step(x_in, gain_attn, gain_mlp, rope_cos, rope_sin, w_q, w_k, w_v, w_o, w_gate, w_up, w_down):
        def rows_of(t):
            return jnp.broadcast_to(t.reshape(8, 1, 8, TOK), (8, 8, 8, TOK)).reshape(ROWS, TOK)

        cos, sin = rows_of(rope_cos), rows_of(rope_sin)
        cos2 = jnp.concatenate([cos, cos], axis=1)
        sin2 = jnp.concatenate([-sin, sin], axis=1)
        def quarters(w):
            return w.reshape(w.shape[0], 2, 2, TOK, -1)

        def row_blocks(w):
            return w.reshape(w.shape[0], -1, 2, 2, TOK, UNIT)

        y = _call(x_in.reshape(TOK, 4096), gain_attn.reshape(2, 1, 4096), gain_mlp.reshape(2, 1, 4096), cos2, sin2,
                  quarters(w_q), quarters(w_k), quarters(w_v), row_blocks(w_o), quarters(w_gate), quarters(w_up), row_blocks(w_down))
        return y.reshape(x_in.shape)

    return jax.shard_map(device_step, mesh=mesh, in_specs=(act, P(), P(), P(), P(), col, col, col, row, col, col, row), out_specs=act, check_vma=False)
```

```python
import functools
import jax
import jax.numpy as jnp
from jax import lax
from jax.experimental import pallas as pl
from jax.experimental.pallas import tpu as pltpu
from jax.sharding import PartitionSpec as P

EPS = 1e-5
MESH = pl.DeviceIdType.MESH
FULL = slice(None)
RING = 4
FAR = 2
LANE = 128
UNIT = 256
ROWS = 512
TOK = 64
WIDE = 4096
HALF = 2048
HID = 896
DROW = 112
HEAD_SCALE = 128 ** -0.5
BOTH = (0, 1)
SIGNS = (1, -1)

N_AT, N_GU, N_DN = 5, 7, 4
KV, O_ITEM = 2, 3
PER_LAYER = N_AT + N_GU + N_DN
N_ITEMS = 2 * PER_LAYER
AHEAD = 2
SELF, NEXT, PAIR, OTHER = range(RING)


def _entry(stage, src, dst, sub, half, way):
    slot = [(v[0] % RING) * RING + v[1] % RING for v in (src, dst)]
    quarters = {(a, b) for a in BOTH for b in BOTH if sub in (a, None) and half in (b, None)}
    return dict(stage=stage, src=slot[0], dst=slot[1], sub=sub, half=half, way=way, q=quarters)


def _plan_all():
    plan = []
    for axis in BOTH:
        for sign in SIGNS:
            sub = (1 - sign) // 2

            def add(stage, along, across, sub, half):
                src = (along, across) if axis == 0 else (across, along)
                dst = (along - sign, across) if axis == 0 else (across, along - sign)
                plan.append(_entry(stage, src, dst, sub, half, (axis, sign)))

            add(0, 0, 0, None, None)
            add(1, -sign, 0, sub, None)
            for k in SIGNS:
                add(1, 0, k, None, axis)
                add(2, -sign, k, sub, axis)
            add(2, 0, FAR, None, axis)
            add(3, -sign, FAR, sub, axis)
    return plan


def _plan_half():
    plan = []

    def add(stage, dz, role, sub, half, way):
        if way in ("next", "pair"):
            to = {SELF: PAIR} if way == "pair" else {SELF: NEXT, PAIR: OTHER}
            dst = (dz, to[role])
        else:
            dst = (dz - way[1], role)
        plan.append(_entry(stage, (dz, role), dst, sub, half, way))

    add(0, 0, SELF, None, None, "pair")
    add(0, 0, SELF, None, None, "next")
    for sign in SIGNS:
        sub, way = (1 - sign) // 2, (0, sign)
        add(0, 0, SELF, None, None, way)
        add(1, -sign, SELF, sub, None, way)
        add(1, 0, NEXT, None, 0, way)
        add(1, 0, PAIR, None, None, way)
        add(2, -sign, NEXT, sub, 0, way)
        add(2, -sign, PAIR, sub, None, way)
        add(2, 0, OTHER, None, 0, way)
        add(3, -sign, OTHER, sub, 0, way)
        add(1, sign, SELF, None, 1, "next")
        add(2, sign, PAIR, None, 1, "next")
    add(1, 0, PAIR, None, None, "next")
    add(2, FAR, SELF, None, 1, "next")
    add(3, FAR, PAIR, None, 1, "next")
    return plan


ALL, SPLIT = _plan_all(), _plan_half()


def _of(plan, stage):
    return [i for i in range(len(plan)) if plan[i]["stage"] == stage]


def _cut(n, size):
    return FULL if n is None else pl.ds(n * size, size)


def body(x_ref, ga_ref, gm_ref, cos_ref, sin_ref, wq, wk, wv, wo, wg, wu, wd, y_ref, at_g, gu_g, dn_g,
         hu, wbuf, dbuf, part, t1, t2, t3, t4, zbuf, qbuf, kbuf, vbuf, obuf, res, acc,
         at_recv, gu_recv, dn_recv, at_send, gu_send, dn_send, ag_recv, ag_send, rs_recv, rs_send, pr_recv, pr_send, w_sem, d_sem):
    f_me = lax.axis_index("fsdp")
    m_me = lax.axis_index("model")
    z, y = lax.div(f_me, RING), lax.rem(f_me, RING)
    x, c = lax.div(m_me, 2), lax.rem(m_me, 2)
    up = lambda v: lax.rem(v + 1, RING)
    dn = lambda v: lax.rem(v + 3, RING)
    sib = 1 - c
    y_next = y + 1 - 2 * lax.rem(y, 2)
    side = lax.div(y, 2)

    dev_of = {"next": (z * RING + y_next, m_me), "pair": (z * RING + 3 - y, m_me)}
    for s, turn in zip(SIGNS, (up, dn)):
        dev_of[0, s] = (turn(z) * RING + y, m_me)
        dev_of[1, s] = (z * RING + turn(y), m_me)
    x_up, x_dn, x_far = up(x), dn(x), lax.rem(x + FAR, RING)
    dev_xu, dev_xd, dev_sib = (f_me, x_up * 2 + c), (f_me, x_dn * 2 + c), (f_me, x * 2 + sib)

    def lanes(n):
        return pl.ds(pl.multiple_of(n * LANE, LANE), LANE)

    def remote(src, dst, send, recv, dev):
        return pltpu.make_async_remote_copy(src_ref=src, dst_ref=dst, send_sem=send, recv_sem=recv, device_id=dev, device_id_type=MESH)

    kinds = {"at": (ALL, at_g, at_recv, at_send), "gu": (SPLIT, gu_g, gu_recv, gu_send), "dn": (SPLIT, dn_g, dn_recv, dn_send)}

    def stream_copy(kind, n, i):
        plan, g, recv, send = kinds[kind]
        p = plan[i]
        a, b = _cut(p["sub"], 1), _cut(p["half"], 1)
        at = p["src"] if p["stage"] else p["dst"]
        return remote(g.at[n, at, a, b], g.at[n, p["dst"], a, b], send.at[n], recv.at[n, i], dev_of[p["way"]])

    def own_unit(w, layer, j):
        return w.at[layer, :, :, :, pl.ds(pl.multiple_of(j * UNIT, UNIT), UNIT)]

    def own_gu(w, layer, j, h):
        return w.at[layer, :, :, :, lanes(h * N_GU + j)]

    def own_dn(layer, k, h):
        return wd.at[layer, h, lax.rem(k, 2), :, :, :, lanes(lax.div(k, 2))]

    def start_own(item):
        layer, pos = lax.div(item, PER_LAYER), lax.rem(item, PER_LAYER)

        def send(kind, n, src, lane=None):
            plan, g, recv, sems = kinds[kind]
            for i in _of(plan, 0):
                way = plan[i]["way"]
                dst = g.at[n, plan[i]["dst"]]
                if lane is not None:
                    dst = dst.at[:, :, :, pl.ds(lane, LANE)]
                remote(src(1 - side if way == "pair" else side), dst, sems.at[n], recv.at[n, i], dev_of[way]).start()

        @pl.when(pos < KV)
        def _():
            send("at", layer * N_AT + pos, lambda h: own_unit(wq, layer, pos))

        @pl.when(pos == KV)
        def _():
            for k, w in enumerate((wk, wv)):
                send("at", layer * N_AT + pos, lambda h: w.at[layer], k * LANE)

        @pl.when(jnp.logical_and(pos >= O_ITEM, pos < N_AT))
        def _():
            send("at", layer * N_AT + pos, lambda h: wo.at[layer, pos - O_ITEM])

        @pl.when(jnp.logical_and(pos >= N_AT, pos < N_AT + N_GU))
        def _():
            j = pos - N_AT
            for k, w in enumerate((wg, wu)):
                send("gu", layer * N_GU + j, lambda h: own_gu(w, layer, j, h), k * LANE)

        @pl.when(pos >= N_AT + N_GU)
        def _():
            k = pos - N_AT - N_GU
            send("dn", layer * N_DN + k, lambda h: own_dn(layer, k, h))

    def serve(kind, n, stage):
        plan = kinds[kind][0]
        waited = set()
        before = _of(plan, stage - 1)
        for i in _of(plan, stage):
            for j in before:
                if j not in waited and plan[j]["dst"] == plan[i]["src"] and plan[j]["q"] & plan[i]["q"]:
                    stream_copy(kind, n, j).wait_recv()
                    waited.add(j)
            stream_copy(kind, n, i).start()
        for j in before:
            if j not in waited:
                stream_copy(kind, n, j).wait_recv()

    def forward(item, stage):
        layer, pos = lax.div(item, PER_LAYER), lax.rem(item, PER_LAYER)

        @pl.when(pos < N_AT)
        def _():
            serve("at", layer * N_AT + pos, stage)

        @pl.when(jnp.logical_and(pos >= N_AT, pos < N_AT + N_GU))
        def _():
            serve("gu", layer * N_GU + pos - N_AT, stage)

        @pl.when(pos >= N_AT + N_GU)
        def _():
            serve("dn", layer * N_DN + pos - N_AT - N_GU, stage)

    def tick(t):
        for lag in range(RING):
            @pl.when(jnp.logical_and(t >= lag, t < N_ITEMS + lag))
            def _():
                forward(t - lag, lag + 1)

            if lag == FAR:
                @pl.when(t + AHEAD < N_ITEMS)
                def _():
                    start_own(t + AHEAD)

    def ag_copy(inst, k):
        slot = lax.rem(inst, 3)
        own, lo, hi, far = (x * 2 + c), (x_dn * 2 + c), (x_up * 2 + c), (x_far * 2 + c)
        s0, s1 = _cut(0, TOK // 2), _cut(1, TOK // 2)
        blk, rows, dev = [
            (own, FULL, dev_sib), (own, FULL, dev_xu), (own, FULL, dev_xd),
            (lo, s0, dev_xu), (hi, s1, dev_xd),
            (lo, FULL, dev_sib), (hi, FULL, dev_sib), (far, FULL, dev_sib)][k]
        ref = hu.at[slot, blk, rows]
        return remote(ref, ref, ag_send.at[inst, k], ag_recv.at[inst, k], dev)

    def ag_start(inst):
        for k in (1, 2, 0):
            ag_copy(inst, k).start()

    def ag_mid(inst):
        for a, b, d in ((1, 3, 5), (2, 4, 6)):
            ag_copy(inst, a).wait_recv()
            ag_copy(inst, b).start()
            ag_copy(inst, d).start()

    def ag_end(inst):
        for k in (3, 4):
            ag_copy(inst, k).wait_recv()
        ag_copy(inst, 7).start()
        for k in (0, 5, 6, 7):
            ag_copy(inst, k).wait_recv()
        for k in range(8):
            ag_copy(inst, k).wait_send()

    def pair_copy(layer, k):
        if k == 0:
            src, dst = hu.at[1, m_me], hu.at[2, m_me]
        else:
            src, dst = part.at[k - 1, 1, x, c], t4.at[k - 1]
        return remote(src, dst, pr_send.at[layer, k], pr_recv.at[layer, k], dev_of["pair"])

    def rs_copy(inst, hh, k, groups):
        g = pl.ds(0, groups)
        lo, hi = _cut(0, TOK // 2), _cut(1, TOK // 2)
        src, dst, dev = [
            (part.at[hh, g, :, sib], t1.at[hh, g], dev_sib),
            (part.at[hh, g, x_far, c, lo], t2.at[hh, g, 0], dev_xu),
            (part.at[hh, g, x_far, c, hi], t2.at[hh, g, 1], dev_xd),
            (part.at[hh, g, x_up, c], t3.at[hh, g, 0], dev_xu),
            (part.at[hh, g, x_dn, c], t3.at[hh, g, 1], dev_xd)][k]
        return remote(src, dst, rs_send.at[inst, hh, k], rs_recv.at[inst, hh, k], dev)

    def rs_core(inst, hh, groups):
        rs_copy(inst, hh, 0, groups).start()

    def rs_far(inst, hh, groups):
        rs_copy(inst, hh, 0, groups).wait_recv()

        def add(xp):
            def one(g, _):
                part[hh, g, xp, c] = part[hh, g, xp, c] + t1[hh, g, xp]
                return 0
            lax.fori_loop(0, groups, one, 0)

        add(x_far)
        for k in (1, 2):
            rs_copy(inst, hh, k, groups).start()
        for xp in (x_up, x_dn, x):
            add(xp)

    def rs_near(inst, hh, groups):
        for b, xp in ((0, x_up), (1, x_dn)):
            rs_copy(inst, hh, 1 + b, groups).wait_recv()
            r = _cut(b, TOK // 2)
            for g in range(groups):
                part[hh, g, xp, c, r] = part[hh, g, xp, c, r] + t2[hh, g, b]
            rs_copy(inst, hh, 3 + b, groups).start()

    def rs_wait(inst, hh, groups):
        for k in (3, 4):
            rs_copy(inst, hh, k, groups).wait_recv()
        for k in range(5):
            rs_copy(inst, hh, k, groups).wait_send()

    def pair_out(layer, hh):
        rs_wait(2 * layer + 1, hh, 2)
        part[hh, 1, x, c] = part[hh, 1, x, c] + t3[hh, 1, 0] + t3[hh, 1, 1]
        pair_copy(layer, hh + 1).start()

    def pair_in(layer, hh):
        pair_copy(layer, hh + 1).wait()

    def rows16(i):
        return pl.ds(pl.multiple_of(i * 16, 16), 16)

    def add_residual(paired):
        def step(i, _):
            r = rows16(i)
            s = [part[hh, 0, x, c, r] + t3[hh, 0, 0, r] + t3[hh, 0, 1, r] for hh in BOTH]
            if paired:
                s = [s[hh] + t4[hh, r] for hh in BOTH]
            cols = [s[hh][:, f * LANE:(f + 1) * LANE] for f in range(16) for hh in BOTH]
            res[r] = (res[r].astype(jnp.float32) + jnp.concatenate(cols, axis=1)).astype(jnp.bfloat16)
            return 0
        lax.fori_loop(0, RING, step, 0)

    def norm_into(slot, gain):
        def step(i, _):
            r = rows16(i)
            v = res[r].astype(jnp.float32)
            ms = jnp.mean(v * v, axis=-1, keepdims=True)
            hu[slot, m_me, r] = (v * lax.rsqrt(ms + EPS) * gain).astype(jnp.bfloat16)
            return 0
        lax.fori_loop(0, RING, step, 0)

    def src_all(rel):
        return lax.rem(z + lax.div(rel, RING), RING) * RING + lax.rem(y + lax.rem(rel, RING), RING)

    def src_split(rel):
        role = lax.rem(rel, RING)
        b = y + lax.rem(role, 2) * (y_next - y)
        return lax.rem(z + lax.div(rel, RING), RING) * RING + b + lax.div(role, 2) * (3 - 2 * b)

    def load_unit(g, n, slot, own, where):
        mine = wbuf.at[slot, f_me]
        if len(own) == 1:
            pltpu.make_async_copy(own[0], mine, w_sem.at[slot]).start()
        else:
            for k in BOTH:
                pltpu.make_async_copy(own[k], mine.at[:, :, :, pl.ds(k * LANE, LANE)], w_sem.at[slot]).start()

        def one(rel, _):
            pltpu.make_async_copy(g.at[n, rel], wbuf.at[slot, where(rel)], w_sem.at[slot]).start()
            return 0
        lax.fori_loop(1, 16, one, 0)

    def wait_unit(slot):
        pltpu.make_async_copy(wbuf.at[slot], wbuf.at[slot], w_sem.at[slot]).wait()

    def load_down(layer, hh):
        for r in BOTH:
            k = 2 * hh + r
            pltpu.make_async_copy(own_dn(layer, k, side), dbuf.at[r, :, :, :, lanes(f_me)], d_sem).start()

            def one(rel, _):
                pltpu.make_async_copy(dn_g.at[layer * N_DN + k, rel], dbuf.at[r, :, :, :, lanes(src_split(rel))], d_sem).start()
                return 0
            lax.fori_loop(1, 16, one, 0)

    def project(slot, ws):
        acc[...] = jnp.zeros_like(acc)

        def step(kk, _):
            lhs = hu[slot, :, :, pl.ds(pl.multiple_of(kk * ROWS, ROWS), ROWS)].reshape(ROWS, ROWS)
            rhs = wbuf[ws, pl.ds(2 * kk, 2)].reshape(ROWS, UNIT)
            acc[...] += jnp.dot(lhs, rhs, preferred_element_type=jnp.float32)
            return 0
        lax.fori_loop(0, 8, step, 0)

    def rows128(i):
        return pl.ds(pl.multiple_of(i * LANE, LANE), LANE)

    def rope_store(lane, dst):
        def step(i, _):
            r = rows128(i)
            v = acc[r, lane:lane + LANE].astype(jnp.bfloat16).astype(jnp.float32)
            dst[r] = (v * cos_ref[r] + pltpu.roll(v, TOK, 1) * sin_ref[r]).astype(jnp.bfloat16)
            return 0
        lax.fori_loop(0, RING, step, 0)

    def qkv(layer):
        base = layer * N_AT
        for u in BOTH:
            load_unit(at_g, base + u, u, [own_unit(wq, layer, u)], src_all)
        load_unit(at_g, base + KV, KV, [wk.at[layer], wv.at[layer]], src_all)
        for u in BOTH:
            wait_unit(u)
            project(0, u)
            for h in BOTH:
                rope_store(h * LANE, qbuf.at[2 * u + h])
        wait_unit(KV)
        project(0, KV)
        rope_store(0, kbuf)
        vbuf[...] = acc[:, LANE:].astype(jnp.bfloat16)
        for u in BOTH:
            load_unit(at_g, base + O_ITEM + u, u, [wo.at[layer, u]], src_all)

    def attention():
        def step(i, _):
            r = rows128(i)
            qi = lax.broadcasted_iota(jnp.int32, (LANE, ROWS), 0) + i * LANE
            ki = lax.broadcasted_iota(jnp.int32, (LANE, ROWS), 1)
            same = ((qi >> 3) & 7) == ((ki >> 3) & 7)
            qpos = (qi >> 6) * 8 + (qi & 7)
            kpos = (ki >> 6) * 8 + (ki & 7)
            ok = jnp.logical_and(same, qpos >= kpos)
            for h in range(RING):
                s = lax.dot_general(qbuf[h, r], kbuf[...], (((1,), (1,)), ((), ())), preferred_element_type=jnp.float32)
                s = jnp.where(ok, s * HEAD_SCALE, -jnp.inf)
                e = jnp.exp(s - jnp.max(s, axis=-1, keepdims=True))
                p = (e / jnp.sum(e, axis=-1, keepdims=True)).astype(jnp.bfloat16)
                o = jnp.dot(p, vbuf[...], preferred_element_type=jnp.float32)
                obuf[r, h * LANE:(h + 1) * LANE] = o.astype(jnp.bfloat16)
            return 0
        lax.fori_loop(0, RING, step, 0)

    def out_proj():
        for u in BOTH:
            wait_unit(u)

        def step(f, _):
            out = sum(jnp.dot(obuf[:, u * UNIT:(u + 1) * UNIT], wbuf[u, f].reshape(UNIT, UNIT), preferred_element_type=jnp.float32) for u in BOTH)
            for hh in BOTH:
                part[hh, 0, :, :, :, lanes(f)] = out[:, hh * LANE:(hh + 1) * LANE].reshape(RING, 2, TOK, LANE)
            return 0
        lax.fori_loop(0, 16, step, 0)

    def gate_up(layer, group):
        def load(j):
            load_unit(gu_g, layer * N_GU + j, lax.rem(j, 2), [own_gu(wg, layer, j, side), own_gu(wu, layer, j, side)], src_split)

        load(0)

        def step(j, _):
            @pl.when(j + 1 < N_GU)
            def _():
                load(j + 1)
            wait_unit(lax.rem(j, 2))
            project(1 + group, lax.rem(j, 2))

            def rows(i, _):
                r = rows128(i)
                hid = jax.nn.silu(acc[r, 0:LANE]) * acc[r, LANE:]
                zbuf[group, r, lanes(j)] = hid.astype(jnp.bfloat16)
                return 0
            lax.fori_loop(0, RING, rows, 0)
            return 0
        lax.fori_loop(0, N_GU, step, 0)

    def down(layer, hh):
        load_down(layer, hh)
        pltpu.make_async_copy(dbuf, dbuf, d_sem).wait()

        def tile(n, _):
            cols = pl.ds(pl.multiple_of(n * UNIT, UNIT), UNIT)
            rhs = dbuf[:, :, :, :, cols].reshape(HID, UNIT)
            for g in BOTH:
                out = jnp.dot(zbuf[g], rhs, preferred_element_type=jnp.float32)
                part[hh, g, :, :, :, cols] = out.reshape(RING, 2, TOK, UNIT)
            return 0
        lax.fori_loop(0, 8, tile, 0)

    barrier = pltpu.get_barrier_semaphore()
    peers = [dev_of[a, s] for a in BOTH for s in SIGNS] + [dev_xu, dev_xd, dev_sib]
    for dev in peers:
        pl.semaphore_signal(barrier, inc=1, device_id=dev, device_id_type=MESH)
    pl.semaphore_wait(barrier, len(peers))

    for item in range(AHEAD):
        start_own(item)
    res[...] = x_ref[...]
    norm_into(0, ga_ref[0])
    ag_start(0)

    def next_layer(layer):
        @pl.when(layer == 0)
        def _():
            norm_into(0, ga_ref[1])
            ag_start(3)

    def each(fn, *args):
        for hh in BOTH:
            fn(args[0], hh, *args[1:])

    hooks = [
        (23, 40, lambda l: (each(pair_in, l), add_residual(True), next_layer(l))),
        (5, 24, lambda l: ag_mid(3 * l)),
        (7, 25, lambda l: (ag_end(3 * l), qkv(l))),
        (8, 25, lambda l: attention()),
        (8, 26, lambda l: (out_proj(), each(rs_core, 2 * l, 1))),
        (9, 26, lambda l: each(rs_far, 2 * l, 1)),
        (10, 27, lambda l: each(rs_near, 2 * l, 1)),
        (11, 28, lambda l: (each(rs_wait, 2 * l, 1), add_residual(False), norm_into(1, gm_ref[l]), pair_copy(l, 0).start(), ag_start(3 * l + 1))),
        (12, 29, lambda l: ag_mid(3 * l + 1)),
        (13, 30, lambda l: (pair_copy(l, 0).wait(), ag_start(3 * l + 2), ag_end(3 * l + 1))),
        (14, 31, lambda l: gate_up(l, 0)),
        (15, 31, lambda l: ag_mid(3 * l + 2)),
        (16, 32, lambda l: (ag_end(3 * l + 2), gate_up(l, 1))),
        (17, 33, lambda l: (down(l, 0), rs_core(2 * l + 1, 0, 2))),
        (18, 35, lambda l: (down(l, 1), rs_core(2 * l + 1, 1, 2), rs_far(2 * l + 1, 0, 2))),
        (19, 36, lambda l: rs_far(2 * l + 1, 1, 2)),
        (20, 37, lambda l: rs_near(2 * l + 1, 0, 2)),
        (21, 38, lambda l: (rs_near(2 * l + 1, 1, 2), pair_out(l, 0))),
        (22, 39, lambda l: pair_out(l, 1)),
    ]

    def step(t, _):
        tick(t)
        for t0, t1_, what in hooks:
            @pl.when(jnp.logical_or(t == t0, t == t1_))
            def _():
                what(jnp.where(t == t1_, 1, 0))
        return 0
    lax.fori_loop(0, 41, step, 0)
    y_ref[...] = res[...]

    for plan, g, _, send in kinds.values():
        def drain(n, _):
            span = g.at[n, pl.ds(0, 15)]
            pltpu.make_async_copy(span, span, send.at[n]).wait()
            return 0
        lax.fori_loop(0, g.shape[0], drain, 0)


def _call(x, ga, gm, cos, sin, *weights):
    bf, f32 = jnp.bfloat16, jnp.float32
    vm = pl.BlockSpec(memory_space=pltpu.VMEM)
    anys = pl.BlockSpec(memory_space=pl.ANY)
    dma = pltpu.SemaphoreType.DMA
    n_at, n_gu, n_dn = 2 * N_AT, 2 * N_GU, 2 * N_DN
    unit = (16, 2, 2, TOK, UNIT)
    return pl.pallas_call(
        body,
        out_shape=(jax.ShapeDtypeStruct((TOK, WIDE), bf), jax.ShapeDtypeStruct((n_at, *unit), bf),
                   jax.ShapeDtypeStruct((n_gu, *unit), bf), jax.ShapeDtypeStruct((n_dn, 16, 2, 2, DROW, LANE), bf)),
        in_specs=[vm] * 5 + [anys] * len(weights),
        out_specs=(vm, anys, anys, anys),
        scratch_shapes=[
            pltpu.VMEM((3, 8, TOK, WIDE), bf),
            pltpu.VMEM((3, *unit), bf),
            pltpu.VMEM((2, 2, 2, DROW, HALF), bf),
            pltpu.VMEM((2, 2, RING, 2, TOK, HALF), f32),
            pltpu.VMEM((2, 2, RING, TOK, HALF), f32),
            pltpu.VMEM((2, 2, 2, TOK // 2, HALF), f32),
            pltpu.VMEM((2, 2, 2, TOK, HALF), f32),
            pltpu.VMEM((2, TOK, HALF), f32),
            pltpu.VMEM((2, ROWS, HID), bf),
            pltpu.VMEM((RING, ROWS, LANE), bf),
            pltpu.VMEM((ROWS, LANE), bf),
            pltpu.VMEM((ROWS, LANE), bf),
            pltpu.VMEM((ROWS, ROWS), bf),
            pltpu.VMEM((TOK, WIDE), bf),
            pltpu.VMEM((ROWS, UNIT), f32),
            dma((n_at, len(ALL))), dma((n_gu, len(SPLIT))), dma((n_dn, len(SPLIT))),
            dma((n_at,)), dma((n_gu,)), dma((n_dn,)),
            dma((6, 8)), dma((6, 8)), dma((RING, 2, 5)), dma((RING, 2, 5)), dma((2, 3)), dma((2, 3)), dma((3,)), dma,
        ],
        compiler_params=pltpu.CompilerParams(collective_id=0, has_side_effects=True, vmem_limit_bytes=63 * 1024 * 1024),
        cost_estimate=pl.CostEstimate(flops=56 * 10 ** 9, bytes_accessed=330 * 10 ** 6, transcendentals=10 ** 7),
    )(x, ga, gm, cos, sin, *weights)[0]


def solution(mesh):
    act = P('fsdp', 'model', None)
    col = P(None, 'fsdp', 'model')
    row = P(None, 'model', 'fsdp')

    def device_step(x_in, gain_attn, gain_mlp, rope_cos, rope_sin, w_q, w_k, w_v, w_o, w_gate, w_up, w_down):
        def rows_of(t):
            return jnp.broadcast_to(t.reshape(8, 1, 8, TOK), (8, 8, 8, TOK)).reshape(ROWS, TOK)

        cos, sin = rows_of(rope_cos), rows_of(rope_sin)
        cos2 = jnp.concatenate([cos, cos], axis=1)
        sin2 = jnp.concatenate([-sin, sin], axis=1)
        def quarters(w):
            return w.reshape(w.shape[0], 2, 2, TOK, -1)


        y = _call(x_in.reshape(TOK, 4096), gain_attn.reshape(2, 1, 4096), gain_mlp.reshape(2, 1, 4096), cos2, sin2,
                  quarters(w_q), quarters(w_k), quarters(w_v), w_o.reshape(2, 2, 2, 2, TOK, UNIT), quarters(w_gate), quarters(w_up), w_down.reshape(2, 2, 2, 2, 2, DROW, UNIT))
        return y.reshape(x_in.shape)

    return jax.shard_map(device_step, mesh=mesh, in_specs=(act, P(), P(), P(), P(), col, col, col, row, col, col, row), out_specs=act, check_vma=False)
```

```python
import functools
import jax
import jax.numpy as jnp
from jax import lax
from jax.experimental import pallas as pl
from jax.experimental.pallas import tpu as pltpu
from jax.sharding import PartitionSpec as P

EPS = 1e-5
MESH = pl.DeviceIdType.MESH
FULL = slice(None)
RING = 4
FAR = 2
LANE = 128
UNIT = 256
ROWS = 512
TOK = 64
WIDE = 4096
HALF = 2048
SUB = 32
GRP = 256
HID = 896
DROW = 112
HEAD_SCALE = 128 ** -0.5
BOTH = (0, 1)
SIGNS = (1, -1)

N_AT, N_GU, N_DN = 5, 7, 4
KV, O_ITEM = 2, 3
PER_LAYER = N_AT + N_GU + N_DN
N_ITEMS = 2 * PER_LAYER
AHEAD = 2
SELF, NEXT, PAIR, OTHER = range(RING)


def _entry(stage, src, dst, sub, half, way):
    slot = [(v[0] % RING) * RING + v[1] % RING for v in (src, dst)]
    quarters = {(a, b) for a in BOTH for b in BOTH if sub in (a, None) and half in (b, None)}
    return dict(stage=stage, src=slot[0], dst=slot[1], sub=sub, half=half, way=way, q=quarters)


def _plan_all():
    plan = []
    for axis in BOTH:
        for sign in SIGNS:
            sub = (1 - sign) // 2

            def add(stage, along, across, sub, half):
                src = (along, across) if axis == 0 else (across, along)
                dst = (along - sign, across) if axis == 0 else (across, along - sign)
                plan.append(_entry(stage, src, dst, sub, half, (axis, sign)))

            add(0, 0, 0, None, None)
            add(1, -sign, 0, sub, None)
            for k in SIGNS:
                add(1, 0, k, None, axis)
                add(2, -sign, k, sub, axis)
            add(2, 0, FAR, None, axis)
            add(3, -sign, FAR, sub, axis)
    return plan


def _plan_half():
    plan = []

    def add(stage, dz, role, sub, half, way):
        if way in ("next", "pair"):
            to = {SELF: PAIR} if way == "pair" else {SELF: NEXT, PAIR: OTHER}
            dst = (dz, to[role])
        else:
            dst = (dz - way[1], role)
        plan.append(_entry(stage, (dz, role), dst, sub, half, way))

    add(0, 0, SELF, None, None, "pair")
    add(0, 0, SELF, None, None, "next")
    for sign in SIGNS:
        sub, way = (1 - sign) // 2, (0, sign)
        add(0, 0, SELF, None, None, way)
        add(1, -sign, SELF, sub, None, way)
        add(1, 0, NEXT, None, 0, way)
        add(1, 0, PAIR, None, None, way)
        add(2, -sign, NEXT, sub, 0, way)
        add(2, -sign, PAIR, sub, None, way)
        add(2, 0, OTHER, None, 0, way)
        add(3, -sign, OTHER, sub, 0, way)
        add(1, sign, SELF, None, 1, "next")
        add(2, sign, PAIR, None, 1, "next")
    add(1, 0, PAIR, None, None, "next")
    add(2, FAR, SELF, None, 1, "next")
    add(3, FAR, PAIR, None, 1, "next")
    return plan


ALL, SPLIT = _plan_all(), _plan_half()


def _of(plan, stage):
    return [i for i in range(len(plan)) if plan[i]["stage"] == stage]


def _cut(n, size):
    return FULL if n is None else pl.ds(n * size, size)


def body(x_ref, ga_ref, gm_ref, cos_ref, sin_ref, wq, wk, wv, wo, wg, wu, wd, y_ref, at_g, gu_g, dn_g,
         hu, wbuf, dbuf, part, t1, t2, t3, t4, zbuf, qbuf, kbuf, vbuf, obuf, res, acc,
         at_recv, gu_recv, dn_recv, at_send, gu_send, dn_send, ag_recv, ag_send, rs_recv, rs_send, pr_recv, pr_send, w_sem, d_sem):
    f_me = lax.axis_index("fsdp")
    m_me = lax.axis_index("model")
    z, y = lax.div(f_me, RING), lax.rem(f_me, RING)
    x, c = lax.div(m_me, 2), lax.rem(m_me, 2)
    up = lambda v: lax.rem(v + 1, RING)
    dn = lambda v: lax.rem(v + 3, RING)
    sib = 1 - c
    y_next = y + 1 - 2 * lax.rem(y, 2)
    side = lax.div(y, 2)

    dev_of = {"next": (z * RING + y_next, m_me), "pair": (z * RING + 3 - y, m_me)}
    for s, turn in zip(SIGNS, (up, dn)):
        dev_of[0, s] = (turn(z) * RING + y, m_me)
        dev_of[1, s] = (z * RING + turn(y), m_me)
    x_up, x_dn, x_far = up(x), dn(x), lax.rem(x + FAR, RING)
    dev_xu, dev_xd, dev_sib = (f_me, x_up * 2 + c), (f_me, x_dn * 2 + c), (f_me, x * 2 + sib)

    def lanes(n):
        return pl.ds(pl.multiple_of(n * LANE, LANE), LANE)

    def remote(src, dst, send, recv, dev):
        return pltpu.make_async_remote_copy(src_ref=src, dst_ref=dst, send_sem=send, recv_sem=recv, device_id=dev, device_id_type=MESH)

    kinds = {"at": (ALL, at_g, at_recv, at_send), "gu": (SPLIT, gu_g, gu_recv, gu_send), "dn": (SPLIT, dn_g, dn_recv, dn_send)}

    def stream_copy(kind, n, i):
        plan, g, recv, send = kinds[kind]
        p = plan[i]
        a, b = _cut(p["sub"], 1), _cut(p["half"], 1)
        at = p["src"] if p["stage"] else p["dst"]
        return remote(g.at[n, at, a, b], g.at[n, p["dst"], a, b], send.at[n], recv.at[n, i], dev_of[p["way"]])

    def own_unit(w, layer, j):
        return w.at[layer, :, :, :, pl.ds(pl.multiple_of(j * UNIT, UNIT), UNIT)]

    def own_gu(w, layer, j, h):
        return w.at[layer, :, :, :, lanes(h * N_GU + j)]

    def own_dn(layer, k, h):
        return wd.at[layer, h, lax.rem(k, 2), :, :, :, lanes(lax.div(k, 2))]

    def start_own(item):
        layer, pos = lax.div(item, PER_LAYER), lax.rem(item, PER_LAYER)

        def send(kind, n, src, lane=None):
            plan, g, recv, sems = kinds[kind]
            for i in _of(plan, 0):
                way = plan[i]["way"]
                dst = g.at[n, plan[i]["dst"]]
                if lane is not None:
                    dst = dst.at[:, :, :, pl.ds(lane, LANE)]
                remote(src(1 - side if way == "pair" else side), dst, sems.at[n], recv.at[n, i], dev_of[way]).start()

        @pl.when(pos < KV)
        def _():
            send("at", layer * N_AT + pos, lambda h: own_unit(wq, layer, pos))

        @pl.when(pos == KV)
        def _():
            for k, w in enumerate((wk, wv)):
                send("at", layer * N_AT + pos, lambda h: w.at[layer], k * LANE)

        @pl.when(jnp.logical_and(pos >= O_ITEM, pos < N_AT))
        def _():
            send("at", layer * N_AT + pos, lambda h: wo.at[layer, pos - O_ITEM])

        @pl.when(jnp.logical_and(pos >= N_AT, pos < N_AT + N_GU))
        def _():
            j = pos - N_AT
            for k, w in enumerate((wg, wu)):
                send("gu", layer * N_GU + j, lambda h: own_gu(w, layer, j, h), k * LANE)

        @pl.when(pos >= N_AT + N_GU)
        def _():
            k = pos - N_AT - N_GU
            send("dn", layer * N_DN + k, lambda h: own_dn(layer, k, h))

    def serve(kind, n, stage):
        plan = kinds[kind][0]
        waited = set()
        before = _of(plan, stage - 1)
        for i in _of(plan, stage):
            for j in before:
                if j not in waited and plan[j]["dst"] == plan[i]["src"] and plan[j]["q"] & plan[i]["q"]:
                    stream_copy(kind, n, j).wait_recv()
                    waited.add(j)
            stream_copy(kind, n, i).start()
        for j in before:
            if j not in waited:
                stream_copy(kind, n, j).wait_recv()

    def forward(item, stage):
        layer, pos = lax.div(item, PER_LAYER), lax.rem(item, PER_LAYER)

        @pl.when(pos < N_AT)
        def _():
            serve("at", layer * N_AT + pos, stage)

        @pl.when(jnp.logical_and(pos >= N_AT, pos < N_AT + N_GU))
        def _():
            serve("gu", layer * N_GU + pos - N_AT, stage)

        @pl.when(pos >= N_AT + N_GU)
        def _():
            serve("dn", layer * N_DN + pos - N_AT - N_GU, stage)

    def tick(u):
        t = lax.div(u, RING)
        for lag in range(RING):
            @pl.when(jnp.logical_and(lax.rem(u, RING) == lag, jnp.logical_and(t >= N_AT + lag, t < N_ITEMS + lag)))
            def _():
                forward(t - lag, lag + 1)

        @pl.when(jnp.logical_and(lax.rem(u, RING) == FAR, t + AHEAD < N_ITEMS))
        def _():
            start_own(t + AHEAD)

    def ag_copy(layer, slot, th, k):
        own, lo, hi, far = (x * 2 + c), (x_dn * 2 + c), (x_up * 2 + c), (x_far * 2 + c)
        s0, s1 = _cut(0, SUB // 2), _cut(1, SUB // 2)
        blk, rows, dev = [
            (own, FULL, dev_sib), (own, FULL, dev_xu), (own, FULL, dev_xd),
            (lo, s0, dev_xu), (hi, s1, dev_xd),
            (lo, FULL, dev_sib), (hi, FULL, dev_sib), (far, FULL, dev_sib)][k]
        ref = hu.at[th, slot, blk, rows]
        return remote(ref, ref, ag_send.at[layer, slot, th, k], ag_recv.at[layer, slot, th, k], dev)

    def ag_start(*inst):
        for k in (1, 2, 0):
            ag_copy(*inst, k).start()

    def ag_mid(*inst):
        for a, b, d in ((1, 3, 5), (2, 4, 6)):
            ag_copy(*inst, a).wait_recv()
            ag_copy(*inst, b).start()
            ag_copy(*inst, d).start()

    def ag_end(*inst):
        for k in (3, 4):
            ag_copy(*inst, k).wait_recv()
        ag_copy(*inst, 7).start()
        for k in (0, 5, 6, 7):
            ag_copy(*inst, k).wait_recv()
        for k in range(8):
            ag_copy(*inst, k).wait_send()

    def pair_tokens(layer, th):
        return remote(hu.at[th, 1, m_me], hu.at[th, 2, m_me], pr_send.at[layer, th, 2], pr_recv.at[layer, th, 2], dev_of["pair"])

    def pair_sums(layer, th, hh):
        return remote(part.at[th, hh, 1, x, c], t4.at[th, hh], pr_send.at[layer, th, hh], pr_recv.at[layer, th, hh], dev_of["pair"])

    def spans(kind):
        return (BOTH, (0,)) if kind == 2 else ((kind,), BOTH)

    def rs_copy(layer, kind, th, k):
        hs, gs = spans(kind)
        h, g = pl.ds(hs[0], len(hs)), pl.ds(0, len(gs))
        lo, hi = _cut(0, SUB // 2), _cut(1, SUB // 2)
        src, dst, dev = [
            (part.at[th, h, g, :, sib], t1.at[th, h, g], dev_sib),
            (part.at[th, h, g, x_far, c, lo], t2.at[th, h, g, 0], dev_xu),
            (part.at[th, h, g, x_far, c, hi], t2.at[th, h, g, 1], dev_xd),
            (part.at[th, h, g, x_up, c], t3.at[th, h, g, 0], dev_xu),
            (part.at[th, h, g, x_dn, c], t3.at[th, h, g, 1], dev_xd)][k]
        return remote(src, dst, rs_send.at[layer, kind, th, k], rs_recv.at[layer, kind, th, k], dev)

    def rs_far(layer, kind, th):
        rs_copy(layer, kind, th, 0).wait_recv()

        def add(xp):
            for h in spans(kind)[0]:
                for g in spans(kind)[1]:
                    part[th, h, g, xp, c] = part[th, h, g, xp, c] + t1[th, h, g, xp]

        add(x_far)
        for k in (1, 2):
            rs_copy(layer, kind, th, k).start()
        for xp in (x_up, x_dn, x):
            add(xp)

    def rs_near(layer, kind, th):
        for b, xp in ((0, x_up), (1, x_dn)):
            rs_copy(layer, kind, th, 1 + b).wait_recv()
            r = _cut(b, SUB // 2)
            for h in spans(kind)[0]:
                for g in spans(kind)[1]:
                    part[th, h, g, xp, c, r] = part[th, h, g, xp, c, r] + t2[th, h, g, b]
            rs_copy(layer, kind, th, 3 + b).start()

    def rs_wait(layer, kind, th):
        for k in (3, 4):
            rs_copy(layer, kind, th, k).wait_recv()
        for k in range(5):
            rs_copy(layer, kind, th, k).wait_send()

    def pair_out(layer, hh, th):
        rs_wait(layer, hh, th)
        part[th, hh, 1, x, c] = part[th, hh, 1, x, c] + t3[th, hh, 1, 0] + t3[th, hh, 1, 1]
        pair_sums(layer, th, hh).start()

    def add_residual(th, paired):
        for b in BOTH:
            r = _cut(b, 16)
            s = [part[th, hh, 0, x, c, r] + t3[th, hh, 0, 0, r] + t3[th, hh, 0, 1, r] for hh in BOTH]
            if paired:
                s = [s[hh] + t4[th, hh, r] for hh in BOTH]
            cols = [s[hh][:, f * LANE:(f + 1) * LANE] for f in range(16) for hh in BOTH]
            res[th, r] = (res[th, r].astype(jnp.float32) + jnp.concatenate(cols, axis=1)).astype(jnp.bfloat16)

    def norm_into(th, slot, gain):
        for b in BOTH:
            r = _cut(b, 16)
            v = res[th, r].astype(jnp.float32)
            ms = jnp.mean(v * v, axis=-1, keepdims=True)
            hu[th, slot, m_me, r] = (v * lax.rsqrt(ms + EPS) * gain).astype(jnp.bfloat16)

    def src_all(rel):
        return lax.rem(z + lax.div(rel, RING), RING) * RING + lax.rem(y + lax.rem(rel, RING), RING)

    def src_split(rel):
        role = lax.rem(rel, RING)
        b = y + lax.rem(role, 2) * (y_next - y)
        return lax.rem(z + lax.div(rel, RING), RING) * RING + b + lax.div(role, 2) * (3 - 2 * b)

    def load_unit(g, n, slot, own, where):
        mine = wbuf.at[slot, f_me]
        if len(own) == 1:
            pltpu.make_async_copy(own[0], mine, w_sem.at[slot]).start()
        else:
            for k in BOTH:
                pltpu.make_async_copy(own[k], mine.at[:, :, :, pl.ds(k * LANE, LANE)], w_sem.at[slot]).start()

        def one(rel, _):
            pltpu.make_async_copy(g.at[n, rel], wbuf.at[slot, where(rel)], w_sem.at[slot]).start()
            return 0
        lax.fori_loop(1, 16, one, 0)

    def wait_unit(slot):
        pltpu.make_async_copy(wbuf.at[slot], wbuf.at[slot], w_sem.at[slot]).wait()

    def load_down(layer, hh):
        for r in BOTH:
            k = 2 * hh + r
            pltpu.make_async_copy(own_dn(layer, k, side), dbuf.at[r, :, :, :, lanes(f_me)], d_sem).start()

            def one(rel, _):
                pltpu.make_async_copy(dn_g.at[layer * N_DN + k, rel], dbuf.at[r, :, :, :, lanes(src_split(rel))], d_sem).start()
                return 0
            lax.fori_loop(1, 16, one, 0)

    def project(lhs, ws):
        return jnp.dot(lhs, wbuf[ws].reshape(WIDE, UNIT), preferred_element_type=jnp.float32)

    def rope_store(lane, dst):
        v = acc[0:GRP, lane:lane + LANE].astype(jnp.bfloat16).astype(jnp.float32)
        dst[...] = (v * cos_ref[...] + pltpu.roll(v, TOK, 1) * sin_ref[...]).astype(jnp.bfloat16)

    def load_qkv(layer):
        base = layer * N_AT
        for u in BOTH:
            load_unit(at_g, base + u, u, [own_unit(wq, layer, u)], src_all)
        load_unit(at_g, base + KV, KV, [wk.at[layer], wv.at[layer]], src_all)

    def qkv(layer, th):
        for u in range(KV + 1):
            wait_unit(u)
            acc[0:GRP] = project(hu[th, 0].reshape(GRP, WIDE), u)
            if u < KV:
                load_unit(at_g, layer * N_AT + O_ITEM + u, u, [wo.at[layer, u]], src_all)
                for h in BOTH:
                    rope_store(h * LANE, qbuf.at[2 * u + h])
        rope_store(0, kbuf)
        vbuf[...] = acc[0:GRP, LANE:].astype(jnp.bfloat16)

    def attention():
        qi = lax.broadcasted_iota(jnp.int32, (GRP, GRP), 0)
        ki = lax.broadcasted_iota(jnp.int32, (GRP, GRP), 1)
        same = ((qi >> 3) & 3) == ((ki >> 3) & 3)
        qpos = (qi >> 5) * 8 + (qi & 7)
        kpos = (ki >> 5) * 8 + (ki & 7)
        ok = jnp.logical_and(same, qpos >= kpos)
        for h in range(RING):
            s = lax.dot_general(qbuf[h], kbuf[...], (((1,), (1,)), ((), ())), preferred_element_type=jnp.float32)
            s = jnp.where(ok, s * HEAD_SCALE, -jnp.inf)
            e = jnp.exp(s - jnp.max(s, axis=-1, keepdims=True))
            p = (e / jnp.sum(e, axis=-1, keepdims=True)).astype(jnp.bfloat16)
            o = jnp.dot(p, vbuf[...], preferred_element_type=jnp.float32)
            obuf[:, h * LANE:(h + 1) * LANE] = o.astype(jnp.bfloat16)

    def cols_of(f):
        return pl.ds(pl.multiple_of(f * UNIT, UNIT), UNIT)

    def out_proj(th):
        for u in BOTH:
            wait_unit(u)

        def step(i, _):
            for e in range(RING):
                f = i * RING + e
                out = sum(jnp.dot(obuf[:, u * UNIT:(u + 1) * UNIT], wbuf[u, f].reshape(UNIT, UNIT), preferred_element_type=jnp.float32) for u in BOTH)
                for hh in BOTH:
                    part[th, hh, 0, :, :, :, lanes(f)] = out[:, hh * LANE:(hh + 1) * LANE].reshape(RING, 2, SUB, LANE)
            return 0
        lax.fori_loop(0, RING, step, 0)

    def load_gu(layer, j):
        load_unit(gu_g, layer * N_GU + j, j % 2 if isinstance(j, int) else 0, [own_gu(wg, layer, j, side), own_gu(wu, layer, j, side)], src_split)

    def gate_up(layer, j0, j1, th):
        for j in range(j0, j1):
            if j + 1 < j1:
                load_gu(layer, j + 1)
            wait_unit(j % 2)
            acc[...] = project(hu[th, 1:3].reshape(ROWS, WIDE), j % 2)
            zbuf[th, :, j * LANE:(j + 1) * LANE] = (jax.nn.silu(acc[:, 0:LANE]) * acc[:, LANE:]).astype(jnp.bfloat16)
        if th == 0:
            load_gu(layer, jnp.where((layer == 1) == (j0 == 0), RING, 0))
        elif j1 < N_GU:
            load_gu(layer, RING)

    def down(th, hh):
        def step(n, _):
            rhs = dbuf[:, :, :, :, cols_of(n)].reshape(HID, UNIT)
            out = jnp.dot(zbuf[th], rhs, preferred_element_type=jnp.float32)
            part[th, hh, :, :, :, :, cols_of(n)] = out.reshape(2, RING, 2, SUB, UNIT)
            return 0
        lax.fori_loop(0, 8, step, 0)

    barrier = pltpu.get_barrier_semaphore()
    peers = [dev_of[a, s] for a in BOTH for s in SIGNS] + [dev_xu, dev_xd, dev_sib]
    for dev in peers:
        pl.semaphore_signal(barrier, inc=1, device_id=dev, device_id_type=MESH)
    pl.semaphore_wait(barrier, len(peers))

    def every(fn):
        lax.fori_loop(0, N_AT, lambda n, _: (fn(n), 0)[1], 0)

    every(start_own)
    for th in BOTH:
        res[th] = x_ref[th]
        norm_into(th, 0, ga_ref[0])
        ag_start(0, 0, th)
    for stage in range(1, RING):
        every(lambda n: serve("at", n, stage))
        if stage == 1:
            for th in BOTH:
                ag_mid(0, 0, th)
        if stage == FAR:
            for k in range(AHEAD):
                start_own(N_AT + k)
    every(lambda n: serve("at", n, RING))

    def attend(l, th):
        ag_end(l, 0, th)
        qkv(l, th)
        attention()
        out_proj(th)
        rs_copy(l, 2, th, 0).start()
        if th == 0:
            load_qkv(l)

    def to_mlp(l, th):
        rs_wait(l, 2, th)
        add_residual(th, False)
        norm_into(th, 1, gm_ref[l])
        pair_tokens(l, th).start()
        ag_start(l, 1, th)

    def mlp_mid(l, th):
        ag_mid(l, 1, th)
        pair_tokens(l, th).wait()
        ag_start(l, 2, th)

    def mlp_far(l, th):
        ag_end(l, 1, th)
        ag_mid(l, 2, th)
        if th == 0:
            load_gu(l, 0)

    def mlp_in(l, j0, j1, th):
        if j0 == 0:
            ag_end(l, 2, th)
        gate_up(l, j0, j1, th)

    def mlp_out(l, hh, th):
        if th == 0:
            load_down(l, hh)
            pltpu.make_async_copy(dbuf, dbuf, d_sem).wait()
        down(th, hh)
        rs_copy(l, hh, th, 0).start()

    def finish(l, th):
        for hh in BOTH:
            pair_sums(l, th, hh).wait()
        add_residual(th, True)

        @pl.when(l == 0)
        def _():
            norm_into(th, 0, ga_ref[1])
            ag_start(1, 0, th)

    def ag_next(l, th):
        @pl.when(l == 1)
        def _():
            ag_mid(1, 0, th)
        if th == 0:
            load_qkv(l)

    hooks = [
        ("90 93 150 152", finish),
        ("78 82 143 144", lambda l, th: pair_out(l, 0, th)),
        ("87 90 148 149", lambda l, th: pair_out(l, 1, th)),
        ("72 75 135 137", lambda l, th: rs_near(l, 0, th)),
        ("81 84 145 146", lambda l, th: rs_near(l, 1, th)),
        ("69 71 132 135", lambda l, th: rs_far(l, 0, th)),
        ("78 80 141 142", lambda l, th: rs_far(l, 1, th)),
        ("67 69 131 132", lambda l, th: mlp_out(l, 0, th)),
        ("75 77 139 140", lambda l, th: mlp_out(l, 1, th)),
        ("50 53 122 127", lambda l, th: mlp_in(l, 0, 4, th)),
        ("41 46 119 125", mlp_far),
        ("59 62 125 129", lambda l, th: mlp_in(l, 4, 7, th)),
        ("37 42 114 121", mlp_mid),
        ("33 38 109 117", to_mlp),
        ("28 33 103 111", lambda l, th: rs_near(l, 2, th)),
        ("24 29 101 104", lambda l, th: rs_far(l, 2, th)),
        ("20 20 95 97", ag_next),
        ("20 24 98 101", attend),
    ]

    def step(t, _):
        tick(t)
        for when, what in hooks:
            u = [int(n) for n in when.split()]
            for th in BOTH:
                @pl.when(jnp.logical_or(t == u[th], t == u[FAR + th]))
                def _():
                    what(jnp.where(t == u[FAR + th], 1, 0), th)
        return 0
    lax.fori_loop(RING * N_AT, 154, step, 0)
    y_ref[...] = res[...]

    for plan, g, _, send in kinds.values():
        def drain(n, _):
            span = g.at[n, pl.ds(0, 15)]
            pltpu.make_async_copy(span, span, send.at[n]).wait()
            return 0
        lax.fori_loop(0, g.shape[0], drain, 0)


def _call(x, ga, gm, cos, sin, *weights):
    bf, f32 = jnp.bfloat16, jnp.float32
    vm = pl.BlockSpec(memory_space=pltpu.VMEM)
    anys = pl.BlockSpec(memory_space=pl.ANY)
    dma = pltpu.SemaphoreType.DMA
    n_at, n_gu, n_dn = 2 * N_AT, 2 * N_GU, 2 * N_DN
    unit = (16, 2, 2, TOK, UNIT)
    return pl.pallas_call(
        body,
        out_shape=(jax.ShapeDtypeStruct((2, SUB, WIDE), bf), jax.ShapeDtypeStruct((n_at, *unit), bf),
                   jax.ShapeDtypeStruct((n_gu, *unit), bf), jax.ShapeDtypeStruct((n_dn, 16, 2, 2, DROW, LANE), bf)),
        in_specs=[vm] * 5 + [anys] * len(weights),
        out_specs=(vm, anys, anys, anys),
        scratch_shapes=[
            pltpu.VMEM((2, 3, 8, SUB, WIDE), bf),
            pltpu.VMEM((3, *unit), bf),
            pltpu.VMEM((2, 2, 2, DROW, HALF), bf),
            pltpu.VMEM((2, 2, 2, RING, 2, SUB, HALF), f32),
            pltpu.VMEM((2, 2, 2, RING, SUB, HALF), f32),
            pltpu.VMEM((2, 2, 2, 2, SUB // 2, HALF), f32),
            pltpu.VMEM((2, 2, 2, 2, SUB, HALF), f32),
            pltpu.VMEM((2, 2, SUB, HALF), f32),
            pltpu.VMEM((2, ROWS, HID), bf),
            pltpu.VMEM((RING, GRP, LANE), bf),
            pltpu.VMEM((GRP, LANE), bf),
            pltpu.VMEM((GRP, LANE), bf),
            pltpu.VMEM((GRP, ROWS), bf),
            pltpu.VMEM((2, SUB, WIDE), bf),
            pltpu.VMEM((ROWS, UNIT), f32),
            dma((n_at, len(ALL))), dma((n_gu, len(SPLIT))), dma((n_dn, len(SPLIT))),
            dma((n_at,)), dma((n_gu,)), dma((n_dn,)),
            dma((2, 3, 2, 8)), dma((2, 3, 2, 8)), dma((2, 3, 2, 5)), dma((2, 3, 2, 5)), dma((2, 2, 3)), dma((2, 2, 3)), dma((3,)), dma,
        ],
        compiler_params=pltpu.CompilerParams(collective_id=0, has_side_effects=True, vmem_limit_bytes=63 * 1024 * 1024),
        cost_estimate=pl.CostEstimate(flops=56 * 10 ** 9, bytes_accessed=330 * 10 ** 6, transcendentals=10 ** 7),
    )(x, ga, gm, cos, sin, *weights)[0]


def solution(mesh):
    act = P('fsdp', 'model', None)
    col = P(None, 'fsdp', 'model')
    row = P(None, 'model', 'fsdp')

    def device_step(x_in, gain_attn, gain_mlp, rope_cos, rope_sin, w_q, w_k, w_v, w_o, w_gate, w_up, w_down):
        def rows_of(t):
            return jnp.broadcast_to(t.reshape(8, 1, 8, TOK), (8, RING, 8, TOK)).reshape(GRP, TOK)

        cos, sin = rows_of(rope_cos), rows_of(rope_sin)
        cos2 = jnp.concatenate([cos, cos], axis=1)
        sin2 = jnp.concatenate([-sin, sin], axis=1)
        def quarters(w):
            return w.reshape(w.shape[0], 2, 2, TOK, -1)


        y = _call(x_in.reshape(2, SUB, WIDE), gain_attn.reshape(2, 1, WIDE), gain_mlp.reshape(2, 1, WIDE), cos2, sin2,
                  quarters(w_q), quarters(w_k), quarters(w_v), w_o.reshape(2, 2, 2, 2, TOK, UNIT), quarters(w_gate), quarters(w_up), w_down.reshape(2, 2, 2, 2, 2, DROW, UNIT))
        return y.reshape(x_in.shape)

    return jax.shard_map(device_step, mesh=mesh, in_specs=(act, P(), P(), P(), P(), col, col, col, row, col, col, row), out_specs=act, check_vma=False)
```

```python
import functools
import jax
import jax.numpy as jnp
from jax import lax
from jax.experimental import pallas as pl
from jax.experimental.pallas import tpu as pltpu
from jax.sharding import PartitionSpec as P

EPS = 1e-5
MESH = pl.DeviceIdType.MESH
FULL = slice(None)
RING = 4
FAR = 2
LANE = 128
UNIT = 256
ROWS = 512
TOK = 64
WIDE = 4096
HALF = 2048
SUB = 32
GRP = 256
HID = 896
DROW = 112
HEAD_SCALE = 128 ** -0.5
BOTH = (0, 1)
SIGNS = (1, -1)

N_AT, N_GU, N_DN = 5, 7, 4
KV, O_ITEM = 2, 3
PER_LAYER = N_AT + N_GU + N_DN
N_ITEMS = 2 * PER_LAYER
AHEAD = 2
SELF, NEXT, PAIR, OTHER = range(RING)


def _entry(stage, src, dst, sub, half, way):
    slot = [(v[0] % RING) * RING + v[1] % RING for v in (src, dst)]
    quarters = {(a, b) for a in BOTH for b in BOTH if sub in (a, None) and half in (b, None)}
    return dict(stage=stage, src=slot[0], dst=slot[1], sub=sub, half=half, way=way, q=quarters)


def _plan_all():
    plan = []
    for axis in BOTH:
        for sign in SIGNS:
            sub = (1 - sign) // 2

            def add(stage, along, across, sub, half):
                src = (along, across) if axis == 0 else (across, along)
                dst = (along - sign, across) if axis == 0 else (across, along - sign)
                plan.append(_entry(stage, src, dst, sub, half, (axis, sign)))

            add(0, 0, 0, None, None)
            add(1, -sign, 0, sub, None)
            for k in SIGNS:
                add(1, 0, k, None, axis)
                add(2, -sign, k, sub, axis)
            add(2, 0, FAR, None, axis)
            add(3, -sign, FAR, sub, axis)
    return plan


def _plan_half():
    plan = []

    def add(stage, dz, role, sub, half, way):
        if way in ("next", "pair"):
            to = {SELF: PAIR} if way == "pair" else {SELF: NEXT, PAIR: OTHER}
            dst = (dz, to[role])
        else:
            dst = (dz - way[1], role)
        plan.append(_entry(stage, (dz, role), dst, sub, half, way))

    add(0, 0, SELF, None, None, "pair")
    add(0, 0, SELF, None, None, "next")
    for sign in SIGNS:
        sub, way = (1 - sign) // 2, (0, sign)
        add(0, 0, SELF, None, None, way)
        add(1, -sign, SELF, sub, None, way)
        add(1, 0, NEXT, None, 0, way)
        add(1, 0, PAIR, None, None, way)
        add(2, -sign, NEXT, sub, 0, way)
        add(2, -sign, PAIR, sub, None, way)
        add(2, 0, OTHER, None, 0, way)
        add(3, -sign, OTHER, sub, 0, way)
        add(1, sign, SELF, None, 1, "next")
        add(2, sign, PAIR, None, 1, "next")
    add(1, 0, PAIR, None, None, "next")
    add(2, FAR, SELF, None, 1, "next")
    add(3, FAR, PAIR, None, 1, "next")
    return plan


ALL, SPLIT = _plan_all(), _plan_half()


def _of(plan, stage):
    return [i for i in range(len(plan)) if plan[i]["stage"] == stage]


def _cut(n, size):
    return FULL if n is None else pl.ds(n * size, size)


def body(x_ref, ga_ref, gm_ref, cos_in, sin_in, wq, wk, wv, wo, wg, wu, wd, y_ref, at_g, gu_g, dn_g,
         hu, wbuf, dbuf, part, t1, t2, t3, t4, t5, cos_ref, sin_ref, zbuf, qbuf, kbuf, vbuf, obuf, res, acc,
         at_recv, gu_recv, dn_recv, at_send, gu_send, dn_send, ag_recv, ag_send, rs_recv, rs_send, pr_recv, pr_send, sw_recv, sw_send, w_sem, d_sem):
    f_me = lax.axis_index("fsdp")
    m_me = lax.axis_index("model")
    z, y = lax.div(f_me, RING), lax.rem(f_me, RING)
    x, c = lax.div(m_me, 2), lax.rem(m_me, 2)
    up = lambda v: lax.rem(v + 1, RING)
    dn = lambda v: lax.rem(v + 3, RING)
    sib = 1 - c
    y_next = y + 1 - 2 * lax.rem(y, 2)
    side = lax.div(y, 2)

    dev_of = {"next": (z * RING + y_next, m_me), "pair": (z * RING + 3 - y, m_me)}
    for s, turn in zip(SIGNS, (up, dn)):
        dev_of[0, s] = (turn(z) * RING + y, m_me)
        dev_of[1, s] = (z * RING + turn(y), m_me)
    x_up, x_dn, x_far = up(x), dn(x), lax.rem(x + FAR, RING)
    dev_xu, dev_xd, dev_sib = (f_me, x_up * 2 + c), (f_me, x_dn * 2 + c), (f_me, x * 2 + sib)

    def lanes(n):
        return pl.ds(pl.multiple_of(n * LANE, LANE), LANE)

    def remote(src, dst, send, recv, dev):
        return pltpu.make_async_remote_copy(src_ref=src, dst_ref=dst, send_sem=send, recv_sem=recv, device_id=dev, device_id_type=MESH)

    kinds = {"at": (ALL, at_g, at_recv, at_send), "gu": (SPLIT, gu_g, gu_recv, gu_send), "dn": (SPLIT, dn_g, dn_recv, dn_send)}

    y_of = {"at": [lax.rem(y + k, RING) for k in range(RING)], "gu": [y, y_next, 3 - y, 3 - y_next]}
    y_of["dn"] = y_of["gu"]

    def slot_of(kind, seen, src):
        return seen // RING * RING + y_of[kind][src % RING]

    def stream_copy(kind, n, i, land=False):
        plan, g, recv, send = kinds[kind]
        p = plan[i]
        a, b = _cut(p["sub"], 1), _cut(p["half"], 1)
        dst = g.at[n, slot_of(kind, p["dst"], p["dst"] if land else p["src"]), a, b]
        src = dst if land else g.at[n, slot_of(kind, p["src"], p["src"]), a, b]
        return remote(src, dst, send.at[n], recv.at[n, i], dev_of[p["way"]])

    def landed(kind, n, i):
        stream_copy(kind, n, i, True).wait_recv()

    def own_unit(w, layer, j):
        return w.at[layer, :, :, :, pl.ds(pl.multiple_of(j * UNIT, UNIT), UNIT)]

    def own_gu(w, layer, j, h):
        return w.at[layer, :, :, :, lanes(h * N_GU + j)]

    def own_dn(layer, k, h):
        return wd.at[layer, h, lax.rem(k, 2), :, :, :, lanes(lax.div(k, 2))]

    def start_own(item):
        layer, pos = lax.div(item, PER_LAYER), lax.rem(item, PER_LAYER)

        def send(kind, n, src, lane=None):
            plan, g, recv, sems = kinds[kind]
            for i in _of(plan, 0):
                way = plan[i]["way"]
                dst = g.at[n, slot_of(kind, plan[i]["dst"], 0)]
                if lane is not None:
                    dst = dst.at[:, :, :, pl.ds(lane, LANE)]
                remote(src(1 - side if way == "pair" else side), dst, sems.at[n], recv.at[n, i], dev_of[way]).start()

        @pl.when(pos < KV)
        def _():
            send("at", layer * N_AT + pos, lambda h: own_unit(wq, layer, pos))

        @pl.when(pos == KV)
        def _():
            for k, w in enumerate((wk, wv)):
                send("at", layer * N_AT + pos, lambda h: w.at[layer], k * LANE)

        @pl.when(jnp.logical_and(pos >= O_ITEM, pos < N_AT))
        def _():
            send("at", layer * N_AT + pos, lambda h: wo.at[layer, pos - O_ITEM])

        @pl.when(jnp.logical_and(pos >= N_AT, pos < N_AT + N_GU))
        def _():
            j = pos - N_AT
            for k, w in enumerate((wg, wu)):
                send("gu", layer * N_GU + j, lambda h: own_gu(w, layer, j, h), k * LANE)

        @pl.when(pos >= N_AT + N_GU)
        def _():
            k = pos - N_AT - N_GU
            send("dn", layer * N_DN + k, lambda h: own_dn(layer, k, h))

    def serve(kind, n, stage):
        plan = kinds[kind][0]
        waited = set()
        before = _of(plan, stage - 1)
        for i in _of(plan, stage):
            for j in before:
                if j not in waited and plan[j]["dst"] == plan[i]["src"] and plan[j]["q"] & plan[i]["q"]:
                    landed(kind, n, j)
                    waited.add(j)
            stream_copy(kind, n, i).start()
        for j in before:
            if j not in waited:
                landed(kind, n, j)

    def forward(item, stage):
        layer, pos = lax.div(item, PER_LAYER), lax.rem(item, PER_LAYER)

        @pl.when(pos < N_AT)
        def _():
            serve("at", layer * N_AT + pos, stage)

        @pl.when(jnp.logical_and(pos >= N_AT, pos < N_AT + N_GU))
        def _():
            serve("gu", layer * N_GU + pos - N_AT, stage)

        @pl.when(pos >= N_AT + N_GU)
        def _():
            serve("dn", layer * N_DN + pos - N_AT - N_GU, stage)

    def tick(u):
        t = lax.div(u, RING)
        for lag in range(RING):
            @pl.when(jnp.logical_and(lax.rem(u, RING) == lag, jnp.logical_and(t >= N_AT + lag, t < N_ITEMS + lag)))
            def _():
                forward(t - lag, lag + 1)

        @pl.when(jnp.logical_and(lax.rem(u, RING) == FAR, t + AHEAD < N_ITEMS))
        def _():
            start_own(t + AHEAD)

    def ag_copy(layer, slot, th, k):
        own, lo, hi, far = (x * 2 + c), (x_dn * 2 + c), (x_up * 2 + c), (x_far * 2 + c)
        s0, s1 = _cut(0, SUB // 2), _cut(1, SUB // 2)
        blk, rows, dev = [
            (own, FULL, dev_sib), (own, FULL, dev_xu), (own, FULL, dev_xd),
            (lo, s0, dev_xu), (hi, s1, dev_xd),
            (lo, FULL, dev_sib), (hi, FULL, dev_sib), (far, FULL, dev_sib)][k]
        ref = hu.at[th, slot, blk, rows]
        return remote(ref, ref, ag_send.at[layer, slot, th, k], ag_recv.at[layer, slot, th, k], dev)

    def ag_start(*inst):
        for k in (1, 2, 0):
            ag_copy(*inst, k).start()

    def ag_mid(*inst):
        for a, b, d in ((1, 3, 5), (2, 4, 6)):
            ag_copy(*inst, a).wait_recv()
            ag_copy(*inst, b).start()
            ag_copy(*inst, d).start()

    def ag_end(*inst):
        for k in (3, 4):
            ag_copy(*inst, k).wait_recv()
        ag_copy(*inst, 7).start()
        for k in (0, 5, 6, 7):
            ag_copy(*inst, k).wait_recv()
        for k in range(8):
            ag_copy(*inst, k).wait_send()

    def pair_tokens(layer, th):
        return remote(hu.at[th, 1, m_me], hu.at[th, 2, m_me], pr_send.at[layer, th, 2], pr_recv.at[layer, th, 2], dev_of["pair"])

    def pair_sums(layer, th, hh):
        return remote(part.at[th, hh, 1, x, c], t4.at[th, hh], pr_send.at[layer, th, hh], pr_recv.at[layer, th, hh], dev_of["pair"])

    def spans(kind):
        return [((0,), BOTH), ((1,), BOTH), (BOTH, (0,)), ((1,), (0,))][kind]

    def swap():
        return remote(part.at[1, 1, 1, :, c], t5, sw_send.at[0], sw_recv.at[0], dev_of["pair"])

    def swap_out(layer):
        rs_copy(layer, 1, 1, 0).wait_recv()
        for g in (1, 0):
            for xp in range(RING):
                part[1, 1, g, xp, c] = part[1, 1, g, xp, c] + t1[1, 1, g, xp]
            if g:
                swap().start()

    def swap_in(layer):
        swap().wait()
        t4[1, 1] = jnp.zeros_like(t4[1, 1])
        for xp in (x_far, x_up, x_dn, x):
            part[1, 1, 0, xp, c] = part[1, 1, 0, xp, c] + t5[xp]
        for k in (1, 2):
            rs_copy(layer, 3, 1, k).start()

    def rs_copy(layer, kind, th, k):
        hs, gs = spans(kind)
        h, g = pl.ds(hs[0], len(hs)), pl.ds(0, len(gs))
        lo, hi = _cut(0, SUB // 2), _cut(1, SUB // 2)
        src, dst, dev = [
            (part.at[th, h, g, :, sib], t1.at[th, h, g], dev_sib),
            (part.at[th, h, g, x_far, c, lo], t2.at[th, h, g, 0], dev_xu),
            (part.at[th, h, g, x_far, c, hi], t2.at[th, h, g, 1], dev_xd),
            (part.at[th, h, g, x_up, c], t3.at[th, h, g, 0], dev_xu),
            (part.at[th, h, g, x_dn, c], t3.at[th, h, g, 1], dev_xd)][k]
        return remote(src, dst, rs_send.at[layer, kind, th, k], rs_recv.at[layer, kind, th, k], dev)

    def rs_far(layer, kind, th):
        rs_copy(layer, kind, th, 0).wait_recv()

        def add(xp):
            for h in spans(kind)[0]:
                for g in spans(kind)[1]:
                    part[th, h, g, xp, c] = part[th, h, g, xp, c] + t1[th, h, g, xp]

        add(x_far)
        for k in (1, 2):
            rs_copy(layer, kind, th, k).start()
        for xp in (x_up, x_dn, x):
            add(xp)

    def rs_near(layer, kind, th):
        for b, xp in ((0, x_up), (1, x_dn)):
            rs_copy(layer, kind, th, 1 + b).wait_recv()
            r = _cut(b, SUB // 2)
            for h in spans(kind)[0]:
                for g in spans(kind)[1]:
                    part[th, h, g, xp, c, r] = part[th, h, g, xp, c, r] + t2[th, h, g, b]
            rs_copy(layer, kind, th, 3 + b).start()

    def rs_wait(layer, kind, th):
        for k in (3, 4):
            rs_copy(layer, kind, th, k).wait_recv()
        for k in range(5):
            rs_copy(layer, 1 if kind == 3 and k == 0 else kind, th, k).wait_send()

    def pair_out(layer, hh, th):
        rs_wait(layer, hh, th)
        part[th, hh, 1, x, c] = part[th, hh, 1, x, c] + t3[th, hh, 1, 0] + t3[th, hh, 1, 1]
        pair_sums(layer, th, hh).start()

    def add_residual(th, paired):
        for b in BOTH:
            r = _cut(b, 16)
            s = [part[th, hh, 0, x, c, r] + t3[th, hh, 0, 0, r] + t3[th, hh, 0, 1, r] for hh in BOTH]
            if paired:
                s = [s[hh] + t4[th, hh, r] for hh in BOTH]
            cols = [s[hh][:, f * LANE:(f + 1) * LANE] for f in range(16) for hh in BOTH]
            res[th, r] = (res[th, r].astype(jnp.float32) + jnp.concatenate(cols, axis=1)).astype(jnp.bfloat16)

    def norm_into(th, slot, gain):
        for b in BOTH:
            r = _cut(b, 16)
            v = res[th, r].astype(jnp.float32)
            ms = jnp.mean(v * v, axis=-1, keepdims=True)
            hu[th, slot, m_me, r] = (v * lax.rsqrt(ms + EPS) * gain).astype(jnp.bfloat16)

    def place(rel):
        yk = lax.rem(y + lax.rem(rel, RING), RING)
        dz = lax.div(rel, RING)
        return dz * RING + yk, lax.rem(z + dz, RING) * RING + yk

    def load_unit(g, n, slot, own):
        mine = wbuf.at[slot, f_me]
        if len(own) == 1:
            pltpu.make_async_copy(own[0], mine, w_sem.at[slot]).start()
        else:
            for k in BOTH:
                pltpu.make_async_copy(own[k], mine.at[:, :, :, pl.ds(k * LANE, LANE)], w_sem.at[slot]).start()
        for k in range(1, RING):
            here, there = place(k)
            pltpu.make_async_copy(g.at[n, here], wbuf.at[slot, there], w_sem.at[slot]).start()
            row = lax.rem(z + k, RING) * RING
            pltpu.make_async_copy(g.at[n, pl.ds(k * RING, RING)], wbuf.at[slot, pl.ds(row, RING)], w_sem.at[slot]).start()

    def wait_unit(slot):
        pltpu.make_async_copy(wbuf.at[slot], wbuf.at[slot], w_sem.at[slot]).wait()

    def load_down(layer, hh):
        for r in BOTH:
            k = 2 * hh + r
            pltpu.make_async_copy(own_dn(layer, k, side), dbuf.at[r, :, :, :, lanes(f_me)], d_sem).start()

            def one(rel, _):
                here, there = place(rel)
                pltpu.make_async_copy(dn_g.at[layer * N_DN + k, here], dbuf.at[r, :, :, :, lanes(there)], d_sem).start()
                return 0
            lax.fori_loop(1, 16, one, 0)

    def project(lhs, ws):
        return jnp.dot(lhs, wbuf[ws].reshape(WIDE, UNIT), preferred_element_type=jnp.float32)

    def rope_store(lane, dst):
        v = acc[0:GRP, lane:lane + LANE].astype(jnp.bfloat16).astype(jnp.float32)
        dst[...] = (v * cos_ref[...] + pltpu.roll(v, TOK, 1) * sin_ref[...]).astype(jnp.bfloat16)

    def load_qkv(layer):
        base = layer * N_AT
        for u in BOTH:
            load_unit(at_g, base + u, u, [own_unit(wq, layer, u)])
        load_unit(at_g, base + KV, KV, [wk.at[layer], wv.at[layer]])

    def qkv(layer, th):
        for u in range(KV + 1):
            wait_unit(u)
            acc[0:GRP] = project(hu[th, 0].reshape(GRP, WIDE), u)
            if u < KV:
                load_unit(at_g, layer * N_AT + O_ITEM + u, u, [wo.at[layer, u]])
                for h in BOTH:
                    rope_store(h * LANE, qbuf.at[2 * u + h])
        rope_store(0, kbuf)
        vbuf[...] = acc[0:GRP, LANE:].astype(jnp.bfloat16)

    def attention():
        qi = lax.broadcasted_iota(jnp.int32, (GRP, GRP), 0)
        ki = lax.broadcasted_iota(jnp.int32, (GRP, GRP), 1)
        same = ((qi >> 3) & 3) == ((ki >> 3) & 3)
        qpos = (qi >> 5) * 8 + (qi & 7)
        kpos = (ki >> 5) * 8 + (ki & 7)
        ok = jnp.logical_and(same, qpos >= kpos)
        for h in range(RING):
            s = lax.dot_general(qbuf[h], kbuf[...], (((1,), (1,)), ((), ())), preferred_element_type=jnp.float32)
            s = jnp.where(ok, s * HEAD_SCALE, -jnp.inf)
            e = jnp.exp(s - jnp.max(s, axis=-1, keepdims=True))
            p = (e / jnp.sum(e, axis=-1, keepdims=True)).astype(jnp.bfloat16)
            o = jnp.dot(p, vbuf[...], preferred_element_type=jnp.float32)
            obuf[:, h * LANE:(h + 1) * LANE] = o.astype(jnp.bfloat16)

    def cols_of(f):
        return pl.ds(pl.multiple_of(f * UNIT, UNIT), UNIT)

    def out_proj(th):
        for u in BOTH:
            wait_unit(u)

        def step(i, _):
            for e in range(RING):
                f = i * RING + e
                out = sum(jnp.dot(obuf[:, u * UNIT:(u + 1) * UNIT], wbuf[u, f].reshape(UNIT, UNIT), preferred_element_type=jnp.float32) for u in BOTH)
                for hh in BOTH:
                    part[th, hh, 0, :, :, :, lanes(f)] = out[:, hh * LANE:(hh + 1) * LANE].reshape(RING, 2, SUB, LANE)
            return 0
        lax.fori_loop(0, RING, step, 0)

    def load_gu(layer, j):
        load_unit(gu_g, layer * N_GU + j, j % 2 if isinstance(j, int) else 0, [own_gu(wg, layer, j, side), own_gu(wu, layer, j, side)])

    def gate_up(layer, j0, j1, th):
        for j in range(j0, j1):
            if j + 1 < j1:
                load_gu(layer, j + 1)
            wait_unit(j % 2)
            acc[...] = project(hu[th, 1:3].reshape(ROWS, WIDE), j % 2)
            zbuf[th, :, j * LANE:(j + 1) * LANE] = (jax.nn.silu(acc[:, 0:LANE]) * acc[:, LANE:]).astype(jnp.bfloat16)
        if th == 0:
            load_gu(layer, jnp.where((layer == 1) == (j0 == 0), RING, 0))
        elif j1 < N_GU:
            load_gu(layer, RING)

    def down(th, hh):
        def step(n, _):
            rhs = dbuf[:, :, :, :, cols_of(n)].reshape(HID, UNIT)
            out = jnp.dot(zbuf[th], rhs, preferred_element_type=jnp.float32)
            part[th, hh, :, :, :, :, cols_of(n)] = out.reshape(2, RING, 2, SUB, UNIT)
            return 0
        lax.fori_loop(0, 8, step, 0)

    barrier = pltpu.get_barrier_semaphore()
    peers = [dev_of[a, s] for a in BOTH for s in SIGNS] + [dev_xu, dev_xd, dev_sib]
    for dev in peers:
        pl.semaphore_signal(barrier, inc=1, device_id=dev, device_id_type=MESH)
    pl.semaphore_wait(barrier, len(peers))

    def every(fn):
        lax.fori_loop(0, N_AT, lambda n, _: (fn(n), 0)[1], 0)

    every(start_own)
    for th in BOTH:
        res[th] = x_ref[th]
        norm_into(th, 0, ga_ref[0:1])
        ag_start(0, 0, th)
    for i in range(8):
        co, si = cos_in[i * 8:(i + 1) * 8], sin_in[i * 8:(i + 1) * 8]
        for b in range(RING):
            r = pl.ds(i * SUB + b * 8, 8)
            cos_ref[r] = jnp.concatenate([co, co], axis=1)
            sin_ref[r] = jnp.concatenate([-si, si], axis=1)
    for stage in range(1, RING):
        every(lambda n: serve("at", n, stage))
        if stage == 1:
            for th in BOTH:
                ag_mid(0, 0, th)
        if stage == FAR:
            for k in range(AHEAD):
                start_own(N_AT + k)
    every(lambda n: serve("at", n, RING))

    def attend(l, th):
        ag_end(l, 0, th)
        qkv(l, th)
        attention()
        out_proj(th)
        rs_copy(l, 2, th, 0).start()
        if th == 0:
            load_qkv(l)

    def to_mlp(l, th):
        rs_wait(l, 2, th)
        add_residual(th, False)
        norm_into(th, 1, gm_ref[pl.ds(l, 1)])
        pair_tokens(l, th).start()
        ag_start(l, 1, th)

    def mlp_mid(l, th):
        ag_mid(l, 1, th)
        pair_tokens(l, th).wait()
        ag_start(l, 2, th)

    def mlp_far(l, th):
        ag_end(l, 1, th)
        ag_mid(l, 2, th)
        if th == 0:
            load_gu(l, 0)

    def mlp_in(l, j0, j1, th):
        if j0 == 0:
            ag_end(l, 2, th)
        gate_up(l, j0, j1, th)

    def mlp_out(l, hh, th):
        if th == 0:
            load_down(l, hh)
            pltpu.make_async_copy(dbuf, dbuf, d_sem).wait()
        down(th, hh)
        rs_copy(l, hh, th, 0).start()

    def finish(l, th):
        pair_sums(l, th, 0).wait()
        if th == 0:
            pair_sums(l, th, 1).wait()
        else:
            @pl.when(l == 0)
            def _():
                pair_sums(l, th, 1).wait()

            @pl.when(l == 1)
            def _():
                rs_wait(l, 3, th)
        add_residual(th, True)

        @pl.when(l == 0)
        def _():
            norm_into(th, 0, ga_ref[1:2])
            ag_start(1, 0, th)

    def ag_next(l, th):
        @pl.when(l == 1)
        def _():
            ag_mid(1, 0, th)
        if th == 0:
            load_qkv(l)

    hooks = [
        ("78 82 145 147", lambda l, th: pair_out(l, 0, th)),
        ("87 90 150 0", lambda l, th: pair_out(l, 1, th)),
        ("72 75 134 144", lambda l, th: rs_near(l, 0, th)),
        ("81 84 146 0", lambda l, th: rs_near(l, 1, th)),
        ("0 0 0 149", lambda l, th: rs_near(l, 3, th)),
        ("90 93 151 152", finish),
        ("69 71 132 140", lambda l, th: rs_far(l, 0, th)),
        ("78 80 143 0", lambda l, th: rs_far(l, 1, th)),
        ("0 0 0 142", lambda l, th: swap_out(l)),
        ("0 0 0 148", lambda l, th: swap_in(l)),
        ("67 69 131 136", lambda l, th: mlp_out(l, 0, th)),
        ("75 77 139 141", lambda l, th: mlp_out(l, 1, th)),
        ("50 53 122 133", lambda l, th: mlp_in(l, 0, 4, th)),
        ("41 46 119 125", mlp_far),
        ("59 62 125 135", lambda l, th: mlp_in(l, 4, 7, th)),
        ("37 42 114 121", mlp_mid),
        ("33 38 109 117", to_mlp),
        ("28 33 103 111", lambda l, th: rs_near(l, 2, th)),
        ("24 29 101 104", lambda l, th: rs_far(l, 2, th)),
        ("20 20 95 97", ag_next),
        ("20 24 98 101", attend),
    ]

    def step(t, _):
        tick(t)
        for when, what in hooks:
            u = [int(n) for n in when.split()]
            for th in [h for h in BOTH if u[h] or u[FAR + h]]:
                @pl.when(jnp.logical_or(t == u[th], t == u[FAR + th]))
                def _():
                    what(jnp.where(t == u[FAR + th], 1, 0), th)
        return 0
    lax.fori_loop(RING * N_AT, 154, step, 0)
    y_ref[...] = res[...]

    for plan, g, _, send in kinds.values():
        def drain(n, _):
            span = g.at[n, pl.ds(0, 15)]
            pltpu.make_async_copy(span, span, send.at[n]).wait()
            return 0
        lax.fori_loop(0, g.shape[0], drain, 0)


def _call(x, ga, gm, cos, sin, *weights):
    bf, f32 = jnp.bfloat16, jnp.float32
    vm = pl.BlockSpec(memory_space=pltpu.VMEM)
    anys = pl.BlockSpec(memory_space=pl.ANY)
    dma = pltpu.SemaphoreType.DMA
    n_at, n_gu, n_dn = 2 * N_AT, 2 * N_GU, 2 * N_DN
    unit = (16, 2, 2, TOK, UNIT)
    return pl.pallas_call(
        body,
        out_shape=(jax.ShapeDtypeStruct((2, SUB, WIDE), bf), jax.ShapeDtypeStruct((n_at, *unit), bf),
                   jax.ShapeDtypeStruct((n_gu, *unit), bf), jax.ShapeDtypeStruct((n_dn, 16, 2, 2, DROW, LANE), bf)),
        in_specs=[vm] * 5 + [anys] * len(weights),
        out_specs=(vm, anys, anys, anys),
        scratch_shapes=[
            pltpu.VMEM((2, 3, 8, SUB, WIDE), bf),
            pltpu.VMEM((3, *unit), bf),
            pltpu.VMEM((2, 2, 2, DROW, HALF), bf),
            pltpu.VMEM((2, 2, 2, RING, 2, SUB, HALF), f32),
            pltpu.VMEM((2, 2, 2, RING, SUB, HALF), f32),
            pltpu.VMEM((2, 2, 2, 2, SUB // 2, HALF), f32),
            pltpu.VMEM((2, 2, 2, 2, SUB, HALF), f32),
            pltpu.VMEM((2, 2, SUB, HALF), f32),
            pltpu.VMEM((RING, SUB, HALF), f32),
            pltpu.VMEM((GRP, LANE), f32),
            pltpu.VMEM((GRP, LANE), f32),
            pltpu.VMEM((2, ROWS, HID), bf),
            pltpu.VMEM((RING, GRP, LANE), bf),
            pltpu.VMEM((GRP, LANE), bf),
            pltpu.VMEM((GRP, LANE), bf),
            pltpu.VMEM((GRP, ROWS), bf),
            pltpu.VMEM((2, SUB, WIDE), bf),
            pltpu.VMEM((ROWS, UNIT), f32),
            dma((n_at, len(ALL))), dma((n_gu, len(SPLIT))), dma((n_dn, len(SPLIT))),
            dma((n_at,)), dma((n_gu,)), dma((n_dn,)),
            dma((2, 3, 2, 8)), dma((2, 3, 2, 8)), dma((2, RING, 2, 5)), dma((2, RING, 2, 5)), dma((2, 2, 3)), dma((2, 2, 3)), dma((1,)), dma((1,)), dma((3,)), dma,
        ],
        compiler_params=pltpu.CompilerParams(collective_id=0, has_side_effects=True, vmem_limit_bytes=63 * 1024 * 1024),
        cost_estimate=pl.CostEstimate(flops=56 * 10 ** 9, bytes_accessed=330 * 10 ** 6, transcendentals=10 ** 7),
    )(x, ga, gm, cos, sin, *weights)[0]


def solution(mesh):
    act = P('fsdp', 'model', None)
    col = P(None, 'fsdp', 'model')
    row = P(None, 'model', 'fsdp')

    def device_step(x_in, gain_attn, gain_mlp, rope_cos, rope_sin, w_q, w_k, w_v, w_o, w_gate, w_up, w_down):
        def quarters(w):
            return w.reshape(w.shape[0], 2, 2, TOK, -1)


        y = _call(x_in.reshape(2, SUB, WIDE), gain_attn, gain_mlp, rope_cos, rope_sin,
                  quarters(w_q), quarters(w_k), quarters(w_v), w_o.reshape(2, 2, 2, 2, TOK, UNIT), quarters(w_gate), quarters(w_up), w_down.reshape(2, 2, 2, 2, 2, DROW, UNIT))
        return y.reshape(x_in.shape)

    return jax.shard_map(device_step, mesh=mesh, in_specs=(act, P(), P(), P(), P(), col, col, col, row, col, col, row), out_specs=act, check_vma=False)
```
